32 devices in a mesh: slab: 4 (over y, core), wide: 8 (over z, x).
Axes of the slice: x: 2, y: 2, z: 4, core: 2. Of those that a mesh axis runs over, the one named last changes fastest.
Arguments:
- spectrum: float32 [1152, 32, 128], P('wide', 'slab'), may hold values from 0 to 1
- sea_mask: int32 [32, 128], P('slab'), may hold values 0 or 1
- courant: float32 [32], replicated, may hold values from 0.05 to 0.7
- slot_owner: int32 [1152], replicated, may hold values from 0 to 1151, each once
- coupling: bfloat16 [1152, 1152], replicated, may hold values from -0.1875 to 0.1875
Outputs:
- evolved: float32 [1152, 32, 128], P('wide', 'slab')
The draws below stay inside these ranges and needn't reach their ends.
Inputs may be any that keep to these rules, and one draw needn't show every extreme that they name: `slot_owner`: each component occurs in exactly one slot; component f * 36 + d has direction d and frequency f. `sea_mask`: 1 marks a sea point.
All inputs are finite; a program needn't handle non-finite values. No bound on the sum of `sea_mask` on one device may be relied on, other than what follows from the above.
Results may differ from the reference program's by a relative error of at most 0.0015.
Values sent between devices are 32-bit elements; how exact they have to be, the bound alone decides.
No kernel may reach another device: no remote copies, remote signals or barrier semaphores. Data moves between devices by JAX's collectives and lax.ppermute only.
A program may use at most 64 MiB of HBM per device.

```python
import math
import jax
import jax.numpy as jnp
from jax import lax

ND = 36
NF = 32
STEPS = 2
NLON = 128
K = 1152
NLAT = 32
N_SLAB = 4


def plant(drawn, key, least, largest):
    longest = drawn.shape.index(max(drawn.shape))
    spots = []
    for shift in (0, 1):
        where = [jax.random.randint(jax.random.fold_in(key, axis), (), 0, length) for axis, length in enumerate(drawn.shape)]
        where[longest] = (where[longest] + shift) % drawn.shape[longest]
        spots.append(tuple(where))
    return drawn.at[spots[0]].set(least).at[spots[1]].set(largest)


def steps_of(rng, extent, shards, least, largest):
    level, own = 1.0, jax.random.fold_in(rng, 6)
    for position, parts in shards:
        steps = jnp.exp(jax.random.uniform(jax.random.fold_in(own, position), (parts,), jnp.float32, least / len(shards), largest / len(shards)))
        level = level * jnp.repeat(steps, extent[position] // parts).reshape([-1 if axis == position else 1 for axis in range(len(extent))])
    return level


def gaussian(rng, shape, scale, reach, held_as=jnp.bfloat16):
    drawn = jax.random.normal(rng, shape, jnp.float32) * scale
    return jnp.minimum(jnp.maximum(drawn, -reach), reach).astype(held_as)


def setup_inputs(seed: int = 0) -> dict:
    streams_of = jax.random.split(jax.random.key(seed), 6)
    spectrum = jnp.clip(1.0 * jax.random.uniform(streams_of[0], (K, NLAT, NLON), jnp.float32) ** steps_of(streams_of[0], (K, NLAT, NLON), ((0, 8), (1, 4)), -0.2, 0.2), 0.0, 1.0)
    sea_mask = plant((jax.random.randint(streams_of[1], (NLAT, NLON), 0, 4) < 3).astype(jnp.int32), jax.random.fold_in(streams_of[1], 1), 0, 1)
    courant = jnp.clip(jnp.exp(jax.random.uniform(streams_of[2], (NF,), jnp.float32, math.log(0.05), math.log(0.7))), 0.05, 0.7)
    slot_owner = jax.random.permutation(streams_of[3], K).astype(jnp.int32)
    coupling = gaussian(streams_of[4], (K, K), K ** -0.5, 0.1875)
    return dict(spectrum=spectrum, sea_mask=sea_mask, courant=courant, slot_owner=slot_owner, coupling=coupling)


time_step = 0.5


def velocities(slot_owner, courant):
    band_count = courant.shape[0]
    heading = slot_owner % ND
    freq_band = slot_owner // ND
    picked = freq_band[:, None] == jnp.arange(band_count, dtype=jnp.int32)[None, :]
    wave_speed = jnp.sum(jnp.where(picked, courant[None, :], 0.0), axis=1)
    wave_angle = heading.astype(jnp.float32) * (2.0 * math.pi / ND)
    return wave_speed * jnp.cos(wave_angle), wave_speed * jnp.sin(wave_angle)


def advect(energy, padded, east_speed, north_speed):
    east_speed = east_speed[:, None, None]
    north_speed = north_speed[:, None, None]
    remain = 1.0 - jnp.abs(east_speed) - jnp.abs(north_speed)
    west_side = jnp.roll(energy, 1, axis=2)
    east_side = jnp.roll(energy, -1, axis=2)
    south_side = padded[:, :-2, :]
    north_side = padded[:, 2:, :]
    result = remain * energy + jnp.maximum(east_speed, 0.0) * west_side
    result = result + jnp.maximum(-east_speed, 0.0) * east_side
    result = result + jnp.maximum(north_speed, 0.0) * south_side
    return result + jnp.maximum(-north_speed, 0.0) * north_side


def interact(moved, slot_table):
    slot_count = moved.shape[0]
    flattened = moved.reshape(slot_count, -1)
    rounded = flattened.astype(jnp.bfloat16)
    square = (flattened * flattened).astype(jnp.bfloat16)
    gain_term = flattened * jnp.dot(slot_table, rounded, preferred_element_type=jnp.float32)
    loss_term = lax.dot_general(slot_table, square, (((0,), (0,)), ((), ())), preferred_element_type=jnp.float32)
    updated = jnp.maximum(flattened + time_step * (gain_term - loss_term), 0.0)
    return updated.reshape(moved.shape)


def reference(spectrum, sea_mask, courant, slot_owner, coupling):
    sea_float = sea_mask.astype(jnp.float32)
    east_speed, north_speed = velocities(slot_owner, courant)
    slot_table = jnp.take(jnp.take(coupling, slot_owner, axis=0), slot_owner, axis=1)
    energy = spectrum * sea_float[None]
    block_rows = NLAT // N_SLAB
    for repeat in range(STEPS):
        padded = jnp.pad(energy, ((0, 0), (1, 1), (0, 0)))
        moved = advect(energy, padded, east_speed, north_speed)

        def one_block(block_index):
            segment = lax.dynamic_slice_in_dim(moved, block_index * block_rows, block_rows, 1)
            return interact(segment, slot_table)

        pieces = lax.map(one_block, jnp.arange(N_SLAB, dtype=jnp.int32))
        energy = jnp.moveaxis(pieces, 0, 1).reshape(moved.shape) * sea_float[None]
    return energy
```

```python
import functools
import math

import jax
import jax.numpy as jnp
import numpy as np
from jax import lax
from jax.experimental import pallas as pl
from jax.experimental.pallas import tpu as pltpu
from jax.sharding import PartitionSpec as P

ND = 36
STEPS = 2
LANES = 128
SUBS = 8

time_step = 0.5


def extended(cells, sides, width):
    for axis, dim in sides:
        count = lax.axis_size(axis)
        ends = count - 1
        head = lax.slice_in_dim(cells, 0, width, axis=dim)
        tail = lax.slice_in_dim(cells, cells.shape[dim] - width, cells.shape[dim], axis=dim)
        cells = jnp.concatenate(
            [
                lax.ppermute(tail, axis, [(i, (i + 1) % count) for i in range(ends)]),
                cells,
                lax.ppermute(head, axis, [((i + 1) % count, i) for i in range(ends)]),
            ],
            axis=dim,
        )
    return cells


def velocities(slot_owner, courant):
    band_count = courant.shape[0]
    heading = slot_owner % ND
    freq_band = slot_owner // ND
    picked = freq_band[:, None] == jnp.arange(band_count, dtype=jnp.int32)[None, :]
    wave_speed = jnp.sum(jnp.where(picked, courant[None, :], 0.0), axis=1)
    wave_angle = heading.astype(jnp.float32) * (2.0 * math.pi / ND)
    return (wave_speed * jnp.cos(wave_angle), wave_speed * jnp.sin(wave_angle))


def combine_sides(energy, west_side, east_side, south_side, north_side, east_speed, north_speed):
    east_speed = east_speed[:, None, None]
    north_speed = north_speed[:, None, None]
    remain = 1.0 - jnp.abs(east_speed) - jnp.abs(north_speed)
    result = remain * energy + jnp.maximum(east_speed, 0.0) * west_side
    result = result + jnp.maximum(-east_speed, 0.0) * east_side
    result = result + jnp.maximum(north_speed, 0.0) * south_side
    return result + jnp.maximum(-north_speed, 0.0) * north_side


def advect(energy, padded, east_speed, north_speed):
    west_side = jnp.roll(energy, 1, axis=2)
    east_side = jnp.roll(energy, -1, axis=2)
    return combine_sides(
        energy, west_side, east_side, padded[:, :-2, :], padded[:, 2:, :], east_speed, north_speed
    )


def interact(moved, slot_table):
    slot_count = moved.shape[0]
    flattened = moved.reshape(slot_count, -1)
    rounded = flattened.astype(jnp.bfloat16)
    square = (flattened * flattened).astype(jnp.bfloat16)
    gain_term = flattened * jnp.dot(slot_table, rounded, preferred_element_type=jnp.float32)
    loss_term = lax.dot_general(
        slot_table, square, (((0,), (0,)), ((), ())), preferred_element_type=jnp.float32
    )
    updated = jnp.maximum(flattened + time_step * (gain_term - loss_term), 0.0)
    return updated.reshape(moved.shape)


def general_body(spectrum, sea_mask, courant, slot_owner, coupling):
    slot_count = spectrum.shape[0]
    wide_index = lax.axis_index("wide")
    sea_float = sea_mask.astype(jnp.float32)
    slot_table = jnp.take(jnp.take(coupling, slot_owner, axis=0), slot_owner, axis=1)
    energy = spectrum * sea_float[None]
    own_slots = lax.dynamic_slice_in_dim(slot_owner, wide_index * slot_count, slot_count, 0)
    east_speed, north_speed = velocities(own_slots, courant)
    for repeat in range(STEPS):
        padded = extended(energy, (("slab", 1),), 1)
        moved = advect(energy, padded, east_speed, north_speed)
        energy = (
            lax.all_to_all(
                interact(
                    lax.all_to_all(moved, "wide", split_axis=1, concat_axis=0, tiled=True),
                    slot_table,
                ),
                "wide",
                split_axis=0,
                concat_axis=1,
                tiled=True,
            )
            * sea_float[None]
        )
    return energy


def ring_order(count):
    ring = list(range(0, count, 2)) + list(range(1, count, 2))[::-1]
    place = [0] * count
    for block, device in enumerate(ring):
        place[device] = block
    return place, ring


def trig_table():
    angle = np.arange(ND, dtype=np.float32) * np.float32(2.0 * math.pi / ND)
    return np.cos(angle), np.sin(angle)


def shares(east, north):
    return (
        1.0 - jnp.abs(east) - jnp.abs(north),
        jnp.maximum(east, 0.0),
        jnp.maximum(-east, 0.0),
        jnp.maximum(north, 0.0),
        jnp.maximum(-north, 0.0),
    )


def swap_lane_blocks(parts, width):
    count = len(parts)
    lane = lax.broadcasted_iota(jnp.int32, parts[0].shape, 1) // width
    bit = 1
    while bit < count:
        low = (lane & bit) == 0
        done = list(parts)
        for a in range(count):
            if a & bit:
                continue
            b = a | bit
            done[a] = jnp.where(low, parts[a], pltpu.roll(parts[b], bit * width, 1))
            done[b] = jnp.where(low, pltpu.roll(parts[a], LANES - bit * width, 1), parts[b])
        parts = done
        bit *= 2
    return parts


def lookup_columns(owner, courant, table):
    lane = lax.broadcasted_iota(jnp.int32, (owner.shape[0], LANES), 1)
    band = owner // ND
    heading = owner - band * ND
    speed = jnp.sum(jnp.where(lane == band, courant, 0.0), axis=1, keepdims=True)
    cosine = jnp.sum(jnp.where(lane == heading, table[0:1], 0.0), axis=1, keepdims=True)
    sine = jnp.sum(jnp.where(lane == heading, table[1:2], 0.0), axis=1, keepdims=True)
    return speed * cosine, speed * sine


def spread_kernel(place, cols, x_ref, sea_ref, prev_ref, next_ref, owner_ref, courant_ref, table_ref, out_ref):
    slots = prev_ref.shape[0]
    courant, table = courant_ref[...], table_ref[...]
    sea = [jnp.broadcast_to(sea_ref[r : r + 1, :], (SUBS, LANES)) for r in range(SUBS)]

    def group(g, carry):
        base = pl.multiple_of(g * SUBS, SUBS)
        here = pl.ds(base, SUBS)
        east, north = lookup_columns(owner_ref[here, :], courant, table)
        remain, west_in, east_in, south_in, north_in = shares(east, north)
        rows = [
            x_ref[pl.ds(base * SUBS + r, SUBS, stride=SUBS), :] * sea[r] for r in range(SUBS)
        ]
        rows = [prev_ref[here, :]] + rows + [next_ref[here, :]]
        moved = []
        for r in range(1, SUBS + 1):
            value = remain * rows[r] + west_in * pltpu.roll(rows[r], 1, 1)
            value = value + east_in * pltpu.roll(rows[r], LANES - 1, 1)
            value = value + south_in * rows[r - 1]
            moved.append(value + north_in * rows[r + 1])
        blocks = swap_lane_blocks(moved, cols)
        for device, block in enumerate(place):
            out_ref[device, here, :] = blocks[block]
        return carry

    lax.fori_loop(0, slots // SUBS, group, 0)


def gather_kernel(ring, cols, x_ref, out_ref):
    slots = x_ref.shape[1]

    def group(g, carry):
        base = pl.multiple_of(g * SUBS, SUBS)
        here = pl.ds(base, SUBS)
        rows = swap_lane_blocks([x_ref[device, here, :] for device in ring], cols)
        for r in range(SUBS):
            out_ref[pl.ds(base * SUBS + r, SUBS, stride=SUBS), :] = rows[r]
        return carry

    lax.fori_loop(0, slots // SUBS, group, 0)


def table_kernel(row_ref, col_ref, coupling_ref, courant_ref, table_ref, out_ref, share_ref, half_ref):
    count = row_ref.shape[1]
    owner = row_ref[...]
    step = LANES
    for c in range(0, count, step):
        line = lax.broadcasted_iota(jnp.int32, (count, step), 0)
        pick = (line == owner[:, c : c + step]).astype(jnp.bfloat16)
        half_ref[:, c : c + step] = jnp.dot(
            coupling_ref[...], pick, preferred_element_type=jnp.float32
        ).astype(jnp.bfloat16)
    for c in range(0, count, step):
        line = lax.broadcasted_iota(jnp.int32, (step, count), 1)
        pick = (line == col_ref[c : c + step, :]).astype(jnp.bfloat16)
        out_ref[c : c + step, :] = jnp.dot(
            pick, half_ref[...], preferred_element_type=jnp.float32
        ).astype(jnp.bfloat16)
    band = owner // ND
    heading = owner - band * ND
    line = lax.broadcasted_iota(jnp.int32, (LANES, count), 0)
    speed = jnp.sum(jnp.where(line == band, courant_ref[...], 0.0), axis=0, keepdims=True)
    cosine = jnp.sum(jnp.where(line == heading, table_ref[:, 0:1], 0.0), axis=0, keepdims=True)
    sine = jnp.sum(jnp.where(line == heading, table_ref[:, 1:2], 0.0), axis=0, keepdims=True)
    for k, share in enumerate(shares(speed * cosine, speed * sine)):
        share_ref[k : k + 1, :] = share


def contract(moved_ref, rounded_ref, square_ref, table_ref, sea, store):
    count = moved_ref.shape[1]
    step = LANES
    for c in range(0, count, step):
        gain = lax.dot_general(
            rounded_ref[...],
            table_ref[c : c + step, :],
            (((1,), (1,)), ((), ())),
            preferred_element_type=jnp.float32,
        )
        loss = jnp.dot(square_ref[...], table_ref[:, c : c + step], preferred_element_type=jnp.float32)
        moved = moved_ref[:, c : c + step]
        store(c, jnp.maximum(moved + time_step * (moved * gain - loss), 0.0) * sea)


def first_kernel(cols, x_ref, table_ref, sea_ref, out_ref, n_ref, s_ref, w_ref, e_ref, moved_ref, rounded_ref, square_ref):
    count, points = x_ref.shape
    step = LANES
    for c in range(0, count, step):
        moved = x_ref[c : c + step, :].T
        moved_ref[:, c : c + step] = moved
        rounded_ref[:, c : c + step] = moved.astype(jnp.bfloat16)
        square_ref[:, c : c + step] = (moved * moved).astype(jnp.bfloat16)

    def store(c, value):
        there = slice(c, c + step)
        out_ref[:, there] = value
        n_ref[:, there] = value[:cols]
        s_ref[:, there] = value[points - cols :]
        for r in range(points // cols):
            w_ref[r : r + 1, there] = value[r * cols : r * cols + 1]
            e_ref[r : r + 1, there] = value[(r + 1) * cols - 1 : (r + 1) * cols]

    contract(moved_ref, rounded_ref, square_ref, table_ref, sea_ref[...], store)


def second_kernel(cols, x_ref, n_ref, s_ref, w_ref, e_ref, share_ref, table_ref, sea_ref, out_ref, moved_ref, rounded_ref, square_ref):
    points, count = x_ref.shape
    step = LANES
    line = lax.broadcasted_iota(jnp.int32, (points, step), 0) % cols
    for c in range(0, count, step):
        there = slice(c, c + step)
        here = x_ref[:, there]
        share = [share_ref[k : k + 1, there] for k in range(5)]

        def along(ref):
            return jnp.concatenate(
                [jnp.broadcast_to(ref[r : r + 1, there], (cols, step)) for r in range(points // cols)], axis=0
            )

        west = jnp.where(line == 0, along(w_ref), pltpu.roll(here, 1, 0))
        east = jnp.where(line == cols - 1, along(e_ref), pltpu.roll(here, points - 1, 0))
        south = jnp.concatenate([s_ref[:, there], here[: points - cols]], axis=0)
        north = jnp.concatenate([here[cols:], n_ref[:, there]], axis=0)
        moved = share[0] * here + share[1] * west
        moved = moved + share[2] * east
        moved = moved + share[3] * south
        moved = moved + share[4] * north
        moved_ref[:, there] = moved
        rounded_ref[:, there] = moved.astype(jnp.bfloat16)
        square_ref[:, there] = (moved * moved).astype(jnp.bfloat16)

    def store(c, value):
        out_ref[c : c + step, :] = value.T

    contract(moved_ref, rounded_ref, square_ref, table_ref, sea_ref[...], store)


def block_body(spectrum, sea_mask, courant, slot_owner, coupling):
    slots, rows, lons = spectrum.shape
    wide, slabs = lax.axis_size("wide"), lax.axis_size("slab")
    count = slots * wide
    cols = lons // wide
    points = rows * cols
    wide_index = lax.axis_index("wide")
    place, ring = ring_order(wide)
    vmem = pl.BlockSpec(memory_space=pltpu.VMEM)
    f32 = jnp.float32

    def call(kernel, name, outs, n_in, scratch=(), flops=0):
        return pl.pallas_call(
            kernel,
            out_shape=outs,
            in_specs=[vmem] * n_in,
            out_specs=jax.tree.map(lambda _: vmem, outs),
            scratch_shapes=scratch,
            cost_estimate=pl.CostEstimate(flops=flops, transcendentals=0, bytes_accessed=0),
            name=name,
        )

    shape = jax.ShapeDtypeStruct
    sea = sea_mask.astype(f32)
    first_row = spectrum[:, 0, :] * sea[0]
    last_row = spectrum[:, rows - 1, :] * sea[rows - 1]
    prev_row = lax.ppermute(last_row, "slab", [(i, i + 1) for i in range(slabs - 1)])
    next_row = lax.ppermute(first_row, "slab", [(i + 1, i) for i in range(slabs - 1)])
    own = lax.dynamic_slice_in_dim(slot_owner, wide_index * slots, slots, 0)
    cosine, sine = trig_table()
    table = np.zeros((SUBS, LANES), np.float32)
    table[0, :ND], table[1, :ND] = cosine, sine
    speeds = jnp.pad(courant, (0, LANES - courant.shape[0]))

    blocks = call(
        functools.partial(spread_kernel, place, cols),
        "spread",
        shape((wide, slots, LANES), f32),
        7,
    )(spectrum.reshape(slots * rows, lons), sea, prev_row, next_row, own[:, None], speeds[None, :], jnp.asarray(table))
    arrived = lax.all_to_all(blocks, "wide", 0, 0).reshape(count, points)

    slot_table, share = call(
        table_kernel,
        "table",
        (shape((count, count), jnp.bfloat16), shape((SUBS, count), f32)),
        5,
        (pltpu.VMEM((count, count), jnp.bfloat16),),
        flops=4 * count**3,
    )(slot_owner[None, :], slot_owner[:, None], coupling, speeds[:, None], jnp.asarray(table.T))

    block_index = jnp.asarray(place, jnp.int32)[wide_index]
    sea_block = lax.dynamic_slice_in_dim(sea, block_index * cols, cols, 1).reshape(points, 1)

    scratch = (
        pltpu.VMEM((points, count), f32),
        pltpu.VMEM((points, count), jnp.bfloat16),
        pltpu.VMEM((points, count), jnp.bfloat16),
    )
    energy, first, last, west, east = call(
        functools.partial(first_kernel, cols),
        "first",
        (
            shape((points, count), f32),
            shape((cols, count), f32),
            shape((cols, count), f32),
            shape((rows, count), f32),
            shape((rows, count), f32),
        ),
        3,
        scratch,
        flops=4 * points * count**2,
    )(arrived, slot_table, sea_block)

    both = ("slab", "wide")
    down = [(s * wide + w, (s + 1) * wide + w) for s in range(slabs - 1) for w in range(wide)]
    up = [(b, a) for a, b in down]
    right = [
        (s * wide + ring[j], s * wide + ring[(j + 1) % wide]) for s in range(slabs) for j in range(wide)
    ]
    left = [(b, a) for a, b in right]
    from_south = lax.ppermute(last, both, down)
    from_north = lax.ppermute(first, both, up)
    from_west = lax.ppermute(east, both, right)
    from_east = lax.ppermute(west, both, left)

    updated = call(
        functools.partial(second_kernel, cols),
        "second",
        shape((count, points), f32),
        8,
        scratch,
        flops=4 * points * count**2,
    )(energy, from_north, from_south, from_west, from_east, share, slot_table, sea_block)
    back = lax.all_to_all(updated.reshape(wide, slots, points), "wide", 0, 0)
    evolved = call(
        functools.partial(gather_kernel, ring, cols),
        "gather",
        shape((slots * rows, lons), f32),
        1,
    )(back)
    return evolved.reshape(slots, rows, lons)


def solution(mesh):
    wide, slabs = mesh.shape["wide"], mesh.shape["slab"]

    def body(spectrum, *rest):
        slots, rows, lons = spectrum.shape
        fits = rows == SUBS and lons == LANES and wide == SUBS and slots % SUBS == 0
        fits = fits and (slots * wide) % LANES == 0
        return (block_body if fits else general_body)(spectrum, *rest)

    return jax.shard_map(
        body,
        mesh=mesh,
        in_specs=(P("wide", "slab", None), P("slab", None), P(), P(), P()),
        out_specs=P("wide", "slab", None),
        check_vma=False,
    )
```

```python
import functools
import math

import jax
import jax.numpy as jnp
import numpy as np
from jax import lax
from jax.experimental import pallas as pl
from jax.experimental.pallas import tpu as pltpu
from jax.sharding import PartitionSpec as P

ND = 36
STEPS = 2
LANES = 128
SUBS = 8
SWAP_ORDER = (4, 6, 5, 7, 3, 1, 2)

time_step = 0.5


def extended(cells, sides, width):
    for axis, dim in sides:
        count = lax.axis_size(axis)
        ends = count - 1
        head = lax.slice_in_dim(cells, 0, width, axis=dim)
        tail = lax.slice_in_dim(cells, cells.shape[dim] - width, cells.shape[dim], axis=dim)
        cells = jnp.concatenate(
            [
                lax.ppermute(tail, axis, [(i, (i + 1) % count) for i in range(ends)]),
                cells,
                lax.ppermute(head, axis, [((i + 1) % count, i) for i in range(ends)]),
            ],
            axis=dim,
        )
    return cells


def velocities(slot_owner, courant):
    band_count = courant.shape[0]
    heading = slot_owner % ND
    freq_band = slot_owner // ND
    picked = freq_band[:, None] == jnp.arange(band_count, dtype=jnp.int32)[None, :]
    wave_speed = jnp.sum(jnp.where(picked, courant[None, :], 0.0), axis=1)
    wave_angle = heading.astype(jnp.float32) * (2.0 * math.pi / ND)
    return (wave_speed * jnp.cos(wave_angle), wave_speed * jnp.sin(wave_angle))


def combine_sides(energy, west_side, east_side, south_side, north_side, east_speed, north_speed):
    east_speed = east_speed[:, None, None]
    north_speed = north_speed[:, None, None]
    remain = 1.0 - jnp.abs(east_speed) - jnp.abs(north_speed)
    result = remain * energy + jnp.maximum(east_speed, 0.0) * west_side
    result = result + jnp.maximum(-east_speed, 0.0) * east_side
    result = result + jnp.maximum(north_speed, 0.0) * south_side
    return result + jnp.maximum(-north_speed, 0.0) * north_side


def advect(energy, padded, east_speed, north_speed):
    west_side = jnp.roll(energy, 1, axis=2)
    east_side = jnp.roll(energy, -1, axis=2)
    return combine_sides(
        energy, west_side, east_side, padded[:, :-2, :], padded[:, 2:, :], east_speed, north_speed
    )


def interact(moved, slot_table):
    slot_count = moved.shape[0]
    flattened = moved.reshape(slot_count, -1)
    rounded = flattened.astype(jnp.bfloat16)
    square = (flattened * flattened).astype(jnp.bfloat16)
    gain_term = flattened * jnp.dot(slot_table, rounded, preferred_element_type=jnp.float32)
    loss_term = lax.dot_general(
        slot_table, square, (((0,), (0,)), ((), ())), preferred_element_type=jnp.float32
    )
    updated = jnp.maximum(flattened + time_step * (gain_term - loss_term), 0.0)
    return updated.reshape(moved.shape)


def general_body(spectrum, sea_mask, courant, slot_owner, coupling):
    slot_count = spectrum.shape[0]
    wide_index = lax.axis_index("wide")
    sea_float = sea_mask.astype(jnp.float32)
    slot_table = jnp.take(jnp.take(coupling, slot_owner, axis=0), slot_owner, axis=1)
    energy = spectrum * sea_float[None]
    own_slots = lax.dynamic_slice_in_dim(slot_owner, wide_index * slot_count, slot_count, 0)
    east_speed, north_speed = velocities(own_slots, courant)
    for repeat in range(STEPS):
        padded = extended(energy, (("slab", 1),), 1)
        moved = advect(energy, padded, east_speed, north_speed)
        energy = (
            lax.all_to_all(
                interact(
                    lax.all_to_all(moved, "wide", split_axis=1, concat_axis=0, tiled=True),
                    slot_table,
                ),
                "wide",
                split_axis=0,
                concat_axis=1,
                tiled=True,
            )
            * sea_float[None]
        )
    return energy


def ring_order(count):
    return list(range(0, count, 2)) + list(range(1, count, 2))[::-1]


def column_block(device, count):
    half = device // 2
    return jnp.where(device % 2 == 0, half, count - 1 - half)


def trig_table():
    angle = np.arange(ND, dtype=np.float32) * np.float32(2.0 * math.pi / ND)
    table = np.zeros((SUBS, LANES), np.float32)
    table[0, :ND], table[1, :ND] = np.cos(angle), np.sin(angle)
    return table[:2]


def pairs(count, odd, closed=False):
    found = [(i, (i + 1) % count) for i in range(odd, count, 2) if closed or i + 1 < count]
    return found + [(b, a) for a, b in found]


def shares(east, north):
    return (
        1.0 - jnp.abs(east) - jnp.abs(north),
        jnp.maximum(east, 0.0),
        jnp.maximum(-east, 0.0),
        jnp.maximum(north, 0.0),
        jnp.maximum(-north, 0.0),
    )


def swap_lane_blocks(parts, width):
    count = len(parts)
    lane = lax.broadcasted_iota(jnp.int32, parts[0].shape, 1) // width
    bit = 1
    while bit < count:
        low = (lane & bit) == 0
        done = list(parts)
        for a in range(count):
            if a & bit:
                continue
            b = a | bit
            done[a] = jnp.where(low, parts[a], pltpu.roll(parts[b], bit * width, 1))
            done[b] = jnp.where(low, pltpu.roll(parts[a], LANES - bit * width, 1), parts[b])
        parts = done
        bit *= 2
    return parts


def chunks(count, step):
    return [(c, min(step, count - c)) for c in range(0, count, step)]


def as_column(row):
    size = row.shape[1]
    line = lax.broadcasted_iota(jnp.int32, (size, size), 0)
    lane = lax.broadcasted_iota(jnp.int32, (size, size), 1)
    column = jnp.sum(jnp.where(line == lane, row, 0.0), axis=1, keepdims=True)
    return jnp.broadcast_to(column, (size, LANES))


def prepare_kernel(wide, cols, x_hbm, mask_hbm, owner_hbm, courant_hbm, table_hbm, a_ref, b_ref, rows_ref, sea_ref, block_ref, share_ref, own_ref, mask_ref, owner_ref, courant_ref, table_ref, row_sem, sem):
    slots = a_ref.shape[0]
    me = lax.axis_index("wide")
    even = lax.axis_index("slab") % 2 == 0
    small = [
        pltpu.make_async_copy(source, target, sem.at[k])
        for k, (source, target) in enumerate(
            ((mask_hbm, mask_ref), (owner_hbm, owner_ref), (courant_hbm, courant_ref), (table_hbm, table_ref))
        )
    ]
    order = (0, SUBS - 1) + tuple(range(1, SUBS - 1))
    large = [pltpu.make_async_copy(x_hbm.at[:, r, :], rows_ref.at[r], row_sem.at[r]) for r in order]
    for copy in small + large:
        copy.start()
    for copy in small:
        copy.wait()
    sea = mask_ref[...].astype(jnp.float32)
    sea_ref[...] = sea
    points = SUBS * cols
    line = lax.broadcasted_iota(jnp.int32, (points, LANES), 0)
    lane = lax.broadcasted_iota(jnp.int32, (points, LANES), 1)
    spread = jnp.concatenate([jnp.broadcast_to(sea[r : r + 1], (cols, LANES)) for r in range(SUBS)], axis=0)
    start = column_block(me, wide) * cols
    mine = jnp.sum(jnp.where(lane == line % cols + start, spread, 0.0), axis=1, keepdims=True)
    block_ref[...] = jnp.broadcast_to(mine, (points, LANES))

    courant = as_column(courant_ref[...])
    cosine_of = as_column(table_ref[0:1, :])
    sine_of = as_column(table_ref[1:2, :])
    bands = lax.broadcasted_iota(jnp.int32, courant.shape, 0)
    headings = lax.broadcasted_iota(jnp.int32, cosine_of.shape, 0)
    lanes = lax.broadcasted_iota(jnp.int32, (slots, LANES), 1)
    nth = lax.broadcasted_iota(jnp.int32, (slots, LANES), 0) + me * slots
    own = [jnp.zeros((slots, LANES), jnp.float32) for _ in range(2)]
    for k in range(owner_ref.shape[0]):
        owner = owner_ref[k : k + 1, :]
        band = owner // ND
        heading = owner - band * ND
        speed = jnp.sum(jnp.where(bands == band, courant, 0.0), axis=0, keepdims=True)
        cosine = jnp.sum(jnp.where(headings == heading, cosine_of, 0.0), axis=0, keepdims=True)
        sine = jnp.sum(jnp.where(headings == heading, sine_of, 0.0), axis=0, keepdims=True)
        both = (speed * cosine, speed * sine)
        for n, share in enumerate(shares(*both)):
            share_ref[n : n + 1, k * LANES : (k + 1) * LANES] = share
        here = lanes + k * LANES == nth
        own = [value + jnp.where(here, one, 0.0) for value, one in zip(own, both)]
    east, north = (jnp.sum(value, axis=1, keepdims=True) for value in own)
    for n, share in enumerate(shares(east, north)):
        own_ref[n] = jnp.broadcast_to(share, (slots, LANES))

    for copy in large:
        copy.wait()
    head = rows_ref[0] * sea[0:1]
    tail = rows_ref[SUBS - 1] * sea[SUBS - 1 : SUBS]
    a_ref[...] = jnp.where(even, tail, head)
    b_ref[...] = jnp.where(even, head, tail)


def spread_kernel(ring, cols, x_ref, sea_ref, a_ref, b_ref, own_ref, out_ref):
    slots = a_ref.shape[0]
    even = lax.axis_index("slab") % 2 == 0
    sea = [jnp.broadcast_to(sea_ref[r : r + 1, :], (SUBS, LANES)) for r in range(SUBS)]
    for base in range(0, slots, SUBS):
        here = slice(base, base + SUBS)
        remain, west_in, east_in, south_in, north_in = (own_ref[k, here, :] for k in range(5))
        rows = [x_ref[r, here, :] * sea[r] for r in range(SUBS)]
        a, b = a_ref[here, :], b_ref[here, :]
        rows = [jnp.where(even, b, a)] + rows + [jnp.where(even, a, b)]
        moved = []
        for r in range(1, SUBS + 1):
            value = remain * rows[r] + west_in * pltpu.roll(rows[r], 1, 1)
            value = value + east_in * pltpu.roll(rows[r], LANES - 1, 1)
            value = value + south_in * rows[r - 1]
            moved.append(value + north_in * rows[r + 1])
        for device, block in zip(ring, swap_lane_blocks(moved, cols)):
            out_ref[device, here, :] = block


def by_device(parts, me):
    bit = 1
    while bit < len(parts):
        flip = (me & bit) != 0
        parts = [jnp.where(flip, parts[k ^ bit], parts[k]) for k in range(len(parts))]
        bit *= 2
    return parts


def gather_kernel(ring, cols, *refs):
    parts, out_hbm, rows_ref, sem = refs[: len(ring)], *refs[len(ring) :]
    slots = rows_ref.shape[1]
    me = lax.axis_index("wide")
    for base in range(0, slots, SUBS):
        here = slice(base, base + SUBS)
        blocks = by_device([part[here, :] for part in parts], me)
        for r, row in enumerate(swap_lane_blocks([blocks[device] for device in ring], cols)):
            rows_ref[r, here, :] = row
    copies = [pltpu.make_async_copy(rows_ref.at[r], out_hbm.at[:, r, :], sem.at[r]) for r in range(SUBS)]
    for copy in copies:
        copy.start()
    for copy in copies:
        copy.wait()


def table_kernel(row_ref, coupling_ref, out_ref, half_ref):
    count = coupling_ref.shape[0]
    for c, step in chunks(count, 2 * LANES):
        line = lax.broadcasted_iota(jnp.int32, (count, LANES), 0)
        pick = jnp.concatenate(
            [(line == row_ref[(c + n) // LANES : (c + n) // LANES + 1, :]).astype(jnp.bfloat16) for n in range(0, step, LANES)],
            axis=1,
        )
        half_ref[:, c : c + step] = jnp.dot(
            coupling_ref[...], pick, preferred_element_type=jnp.float32
        ).astype(jnp.bfloat16)
    lane = lax.broadcasted_iota(jnp.int32, (LANES, LANES), 1)
    line = lax.broadcasted_iota(jnp.int32, (LANES, LANES), 0)
    for k in range(row_ref.shape[0]):
        owner = row_ref[k : k + 1, :].astype(jnp.float32)
        column = jnp.sum(jnp.where(line == lane, owner, 0.0), axis=1, keepdims=True).astype(jnp.int32)
        pick = (lax.broadcasted_iota(jnp.int32, (LANES, count), 1) == column).astype(jnp.bfloat16)
        out_ref[k * LANES : (k + 1) * LANES, :] = jnp.dot(
            pick, half_ref[...], preferred_element_type=jnp.float32
        ).astype(jnp.bfloat16)


def contract(moved_ref, rounded_ref, square_ref, table_ref, sea, store):
    count = moved_ref.shape[1]
    for c, step in chunks(count, 2 * LANES):
        gain = lax.dot_general(
            rounded_ref[...],
            table_ref[c : c + step, :],
            (((1,), (1,)), ((), ())),
            preferred_element_type=jnp.float32,
        )
        loss = jnp.dot(square_ref[...], table_ref[:, c : c + step], preferred_element_type=jnp.float32)
        for n in range(0, step, LANES):
            moved = moved_ref[:, c + n : c + n + LANES]
            value = moved + time_step * (moved * gain[:, n : n + LANES] - loss[:, n : n + LANES])
            store(c + n, jnp.maximum(value, 0.0) * sea)


def first_kernel(wide, cols, x_ref, table_ref, sea_ref, out_ref, a_ref, b_ref, c_ref, d_ref, moved_ref, rounded_ref, square_ref, value_ref):
    count, points = x_ref.shape
    row_even = lax.axis_index("slab") % 2 == 0
    col_even = column_block(lax.axis_index("wide"), wide) % 2 == 0
    for c in range(0, count, LANES):
        there = slice(c, c + LANES)
        moved = x_ref[there, :].T
        moved_ref[:, there] = moved
        rounded_ref[:, there] = moved.astype(jnp.bfloat16)
        square_ref[:, there] = (moved * moved).astype(jnp.bfloat16)

    def store(c, value):
        there = slice(c, c + LANES)
        out_ref[:, there] = value
        head, tail = value[:cols], value[points - cols :]
        a_ref[:, there] = jnp.where(row_even, tail, head)
        b_ref[:, there] = jnp.where(row_even, head, tail)
        value_ref[...] = value
        west = value_ref[pl.ds(0, points // cols, stride=cols), :]
        east = value_ref[pl.ds(cols - 1, points // cols, stride=cols), :]
        c_ref[:, there] = jnp.where(col_even, east, west)
        d_ref[:, there] = jnp.where(col_even, west, east)

    contract(moved_ref, rounded_ref, square_ref, table_ref, sea_ref[...], store)


def second_kernel(wide, cols, x_ref, a_ref, b_ref, c_ref, d_ref, share_ref, table_ref, sea_ref, *refs):
    outs, (moved_ref, rounded_ref, square_ref, value_ref) = refs[:wide], refs[wide:]
    points, count = x_ref.shape
    row_even = lax.axis_index("slab") % 2 == 0
    col_even = column_block(lax.axis_index("wide"), wide) % 2 == 0
    line = lax.broadcasted_iota(jnp.int32, (points, LANES), 0) % cols
    for c in range(0, count, LANES):
        there = slice(c, c + LANES)
        here = x_ref[:, there]
        share = [share_ref[k : k + 1, there] for k in range(5)]
        a, b, side_c, side_d = a_ref[:, there], b_ref[:, there], c_ref[:, there], d_ref[:, there]

        def along(edge):
            return jnp.concatenate(
                [jnp.broadcast_to(edge[r : r + 1], (cols, LANES)) for r in range(points // cols)], axis=0
            )

        west_edge = along(jnp.where(col_even, side_d, side_c))
        east_edge = along(jnp.where(col_even, side_c, side_d))
        west = jnp.where(line == 0, west_edge, pltpu.roll(here, 1, 0))
        east = jnp.where(line == cols - 1, east_edge, pltpu.roll(here, points - 1, 0))
        south = jnp.concatenate([jnp.where(row_even, b, a), here[: points - cols]], axis=0)
        north = jnp.concatenate([here[cols:], jnp.where(row_even, a, b)], axis=0)
        moved = share[0] * here + share[1] * west
        moved = moved + share[2] * east
        moved = moved + share[3] * south
        moved = moved + share[4] * north
        moved_ref[:, there] = moved
        rounded_ref[:, there] = moved.astype(jnp.bfloat16)
        square_ref[:, there] = (moved * moved).astype(jnp.bfloat16)

    def store(c, value):
        value_ref[c : c + LANES, :] = value.T

    contract(moved_ref, rounded_ref, square_ref, table_ref, sea_ref[...], store)
    slots = count // wide
    me = lax.axis_index("wide")
    for k, out in zip((0,) + SWAP_ORDER, outs):
        out[...] = value_ref[pl.ds(pl.multiple_of((me ^ k) * slots, SUBS), slots), :]


def block_body(spectrum, sea_mask, courant, slot_owner, coupling):
    slots, rows, lons = spectrum.shape
    wide, slabs = lax.axis_size("wide"), lax.axis_size("slab")
    count = slots * wide
    cols = lons // wide
    points = rows * cols
    ring = ring_order(wide)
    vmem = pl.BlockSpec(memory_space=pltpu.VMEM)
    in_hbm = pl.BlockSpec(memory_space=pltpu.HBM)
    f32, bf16 = jnp.float32, jnp.bfloat16
    shape = jax.ShapeDtypeStruct

    def call(kernel, name, outs, ins, scratch=(), flops=0, on_chip_result=True):
        made = pl.pallas_call(
            kernel,
            out_shape=jax.tree.map(lambda out: pltpu.VMEM(out.shape, out.dtype), outs) if on_chip_result else outs,
            in_specs=ins,
            out_specs=jax.tree.map(lambda _: vmem if on_chip_result else in_hbm, outs),
            scratch_shapes=scratch,
            compiler_params=pltpu.CompilerParams(vmem_limit_bytes=24 << 20),
            cost_estimate=pl.CostEstimate(flops=flops, transcendentals=0, bytes_accessed=0),
            name=name,
        )

        def on_chip(*given):
            return made(
                *(
                    pltpu.with_memory_space_constraint(one, spec.memory_space)
                    for one, spec in zip(given, ins)
                )
            )

        return on_chip

    owners = slot_owner.reshape(count // LANES, LANES)
    edge = shape((slots, LANES), f32)
    table = trig_table()
    send_a, send_b, lines, sea, sea_block, share, own = call(
        functools.partial(prepare_kernel, wide, cols),
        "prepare",
        (
            edge,
            edge,
            shape((rows, slots, LANES), f32),
            shape((rows, LANES), f32),
            shape((points, LANES), f32),
            shape((SUBS, count), f32),
            shape((5, slots, LANES), f32),
        ),
        [in_hbm] * 5,
        (
            pltpu.VMEM(sea_mask.shape, jnp.int32),
            pltpu.VMEM(owners.shape, jnp.int32),
            pltpu.VMEM((1,) + courant.shape, f32),
            pltpu.VMEM(table.shape, f32),
            pltpu.SemaphoreType.DMA((rows,)),
            pltpu.SemaphoreType.DMA((4,)),
        ),
    )(spectrum, sea_mask, owners, courant[None, :], jnp.asarray(table))

    def swap_rows(a, b):
        return lax.ppermute(a, "slab", pairs(slabs, 0)), lax.ppermute(b, "slab", pairs(slabs, 1))

    def swap_cols(c, d):
        def along(odd):
            return [(ring[i], ring[j]) for i, j in pairs(wide, odd, closed=True)]

        return lax.ppermute(c, "wide", along(0)), lax.ppermute(d, "wide", along(1))

    blocks = call(
        functools.partial(spread_kernel, ring, cols), "spread", shape((wide, slots, LANES), f32), [vmem] * 5
    )(lines, sea, *swap_rows(send_a, send_b), own)
    arrived = lax.all_to_all(blocks, "wide", 0, 0).reshape(count, points)

    slot_table = call(
        table_kernel,
        "table",
        shape((count, count), bf16),
        [vmem] * 2,
        (pltpu.VMEM((count, count), bf16),),
        flops=4 * count**3,
    )(owners, coupling)

    scratch = (pltpu.VMEM((points, count), f32), pltpu.VMEM((points, count), bf16), pltpu.VMEM((points, count), bf16))
    energy, send_a, send_b, send_c, send_d = call(
        functools.partial(first_kernel, wide, cols),
        "first",
        (shape((points, count), f32),) + (shape((cols, count), f32),) * 2 + (shape((rows, count), f32),) * 2,
        [vmem] * 3,
        scratch + (pltpu.VMEM((points, LANES), f32),),
        flops=4 * points * count**2,
    )(arrived, slot_table, sea_block)
    halos = swap_rows(send_a, send_b) + swap_cols(send_c, send_d)
    updated = call(
        functools.partial(second_kernel, wide, cols),
        "second",
        (edge,) * wide,
        [vmem] * 8,
        scratch + (pltpu.VMEM((count, points), f32),),
        flops=4 * points * count**2,
    )(energy, *halos, share, slot_table, sea_block)
    back = [updated[0]] + [None] * (wide - 1)
    for k, block in zip(SWAP_ORDER, updated[1:]):
        back[k] = lax.ppermute(block, "wide", [(w, w ^ k) for w in range(wide)])
    return call(
        functools.partial(gather_kernel, ring, cols),
        "gather",
        shape((slots, rows, lons), f32),
        [vmem] * wide,
        (pltpu.VMEM((rows, slots, LANES), f32), pltpu.SemaphoreType.DMA((rows,))),
        on_chip_result=False,
    )(*back)


def solution(mesh):
    wide, slabs = mesh.shape["wide"], mesh.shape["slab"]

    def body(spectrum, *rest):
        slots, rows, lons = spectrum.shape
        fits = rows == SUBS and lons == LANES and wide == SUBS and slots % SUBS == 0
        fits = fits and (slots * wide) % LANES == 0
        return (block_body if fits else general_body)(spectrum, *rest)

    return jax.shard_map(
        body,
        mesh=mesh,
        in_specs=(P("wide", "slab", None), P("slab", None), P(), P(), P()),
        out_specs=P("wide", "slab", None),
        check_vma=False,
    )
```

```python
import functools
import math

import jax
import jax.numpy as jnp
import numpy as np
from jax import lax
from jax.experimental import pallas as pl
from jax.experimental.pallas import tpu as pltpu
from jax.sharding import PartitionSpec as P

ND = 36
STEPS = 2
LANES = 128
SUBS = 8
SWAP_ORDER = (4, 1, 6, 2, 5, 3, 7)

time_step = 0.5


def extended(cells, sides, width):
    for axis, dim in sides:
        count = lax.axis_size(axis)
        ends = count - 1
        head = lax.slice_in_dim(cells, 0, width, axis=dim)
        tail = lax.slice_in_dim(cells, cells.shape[dim] - width, cells.shape[dim], axis=dim)
        cells = jnp.concatenate(
            [
                lax.ppermute(tail, axis, [(i, (i + 1) % count) for i in range(ends)]),
                cells,
                lax.ppermute(head, axis, [((i + 1) % count, i) for i in range(ends)]),
            ],
            axis=dim,
        )
    return cells


def velocities(slot_owner, courant):
    band_count = courant.shape[0]
    heading = slot_owner % ND
    freq_band = slot_owner // ND
    picked = freq_band[:, None] == jnp.arange(band_count, dtype=jnp.int32)[None, :]
    wave_speed = jnp.sum(jnp.where(picked, courant[None, :], 0.0), axis=1)
    wave_angle = heading.astype(jnp.float32) * (2.0 * math.pi / ND)
    return (wave_speed * jnp.cos(wave_angle), wave_speed * jnp.sin(wave_angle))


def combine_sides(energy, west_side, east_side, south_side, north_side, east_speed, north_speed):
    east_speed = east_speed[:, None, None]
    north_speed = north_speed[:, None, None]
    remain = 1.0 - jnp.abs(east_speed) - jnp.abs(north_speed)
    result = remain * energy + jnp.maximum(east_speed, 0.0) * west_side
    result = result + jnp.maximum(-east_speed, 0.0) * east_side
    result = result + jnp.maximum(north_speed, 0.0) * south_side
    return result + jnp.maximum(-north_speed, 0.0) * north_side


def advect(energy, padded, east_speed, north_speed):
    west_side = jnp.roll(energy, 1, axis=2)
    east_side = jnp.roll(energy, -1, axis=2)
    return combine_sides(
        energy, west_side, east_side, padded[:, :-2, :], padded[:, 2:, :], east_speed, north_speed
    )


def interact(moved, slot_table):
    slot_count = moved.shape[0]
    flattened = moved.reshape(slot_count, -1)
    rounded = flattened.astype(jnp.bfloat16)
    square = (flattened * flattened).astype(jnp.bfloat16)
    gain_term = flattened * jnp.dot(slot_table, rounded, preferred_element_type=jnp.float32)
    loss_term = lax.dot_general(
        slot_table, square, (((0,), (0,)), ((), ())), preferred_element_type=jnp.float32
    )
    updated = jnp.maximum(flattened + time_step * (gain_term - loss_term), 0.0)
    return updated.reshape(moved.shape)


def general_body(spectrum, sea_mask, courant, slot_owner, coupling):
    slot_count = spectrum.shape[0]
    wide_index = lax.axis_index("wide")
    sea_float = sea_mask.astype(jnp.float32)
    slot_table = jnp.take(jnp.take(coupling, slot_owner, axis=0), slot_owner, axis=1)
    energy = spectrum * sea_float[None]
    own_slots = lax.dynamic_slice_in_dim(slot_owner, wide_index * slot_count, slot_count, 0)
    east_speed, north_speed = velocities(own_slots, courant)
    for repeat in range(STEPS):
        padded = extended(energy, (("slab", 1),), 1)
        moved = advect(energy, padded, east_speed, north_speed)
        energy = (
            lax.all_to_all(
                interact(
                    lax.all_to_all(moved, "wide", split_axis=1, concat_axis=0, tiled=True),
                    slot_table,
                ),
                "wide",
                split_axis=0,
                concat_axis=1,
                tiled=True,
            )
            * sea_float[None]
        )
    return energy


def ring_order(count):
    return list(range(0, count, 2)) + list(range(1, count, 2))[::-1]


def column_block(device, count):
    half = device // 2
    return jnp.where(device % 2 == 0, half, count - 1 - half)


def trig_table():
    angle = np.arange(ND, dtype=np.float32) * np.float32(2.0 * math.pi / ND)
    table = np.zeros((SUBS, LANES), np.float32)
    table[0, :ND], table[1, :ND] = np.cos(angle), np.sin(angle)
    return table[:2]


def pairs(count, odd, closed=False):
    found = [(i, (i + 1) % count) for i in range(odd, count, 2) if closed or i + 1 < count]
    return found + [(b, a) for a, b in found]


def shares(east, north):
    return (
        1.0 - jnp.abs(east) - jnp.abs(north),
        jnp.maximum(east, 0.0),
        jnp.maximum(-east, 0.0),
        jnp.maximum(north, 0.0),
        jnp.maximum(-north, 0.0),
    )


def swap_lane_blocks(parts, width):
    count = len(parts)
    lane = lax.broadcasted_iota(jnp.int32, parts[0].shape, 1)
    bit = 1
    while bit < count:
        low = (lane & (bit * width)) == 0
        other = lane ^ (bit * width)
        done = list(parts)
        for a in range(count):
            if a & bit:
                continue
            b = a | bit
            crossed = jnp.take_along_axis(jnp.where(low, parts[b], parts[a]), other, axis=1)
            done[a] = jnp.where(low, parts[a], crossed)
            done[b] = jnp.where(low, crossed, parts[b])
        parts = done
        bit *= 2
    return parts


def chunks(count, step):
    return [(c, min(step, count - c)) for c in range(0, count, step)]


def as_column(row):
    size = row.shape[1]
    line = lax.broadcasted_iota(jnp.int32, (size, size), 0)
    lane = lax.broadcasted_iota(jnp.int32, (size, size), 1)
    column = jnp.sum(jnp.where(line == lane, row, 0.0), axis=1, keepdims=True)
    return jnp.broadcast_to(column, (size, LANES))


def prepare_kernel(wide, cols, x_hbm, mask_hbm, owner_hbm, courant_hbm, table_hbm, a_ref, b_ref, rows_ref, sea_ref, block_ref, share_ref, own_ref, mask_ref, owner_ref, courant_ref, table_ref, row_sem, sem):
    slots = a_ref.shape[0]
    me = lax.axis_index("wide")
    even = lax.axis_index("slab") % 2 == 0
    small = [
        pltpu.make_async_copy(source, target, sem.at[k])
        for k, (source, target) in enumerate(
            ((mask_hbm, mask_ref), (owner_hbm, owner_ref), (courant_hbm, courant_ref), (table_hbm, table_ref))
        )
    ]
    order = (0, SUBS - 1) + tuple(range(1, SUBS - 1))
    large = [pltpu.make_async_copy(x_hbm.at[:, r, :], rows_ref.at[r], row_sem.at[r]) for r in order]
    for copy in small + large:
        copy.start()
    for copy in small:
        copy.wait()
    sea = mask_ref[...].astype(jnp.float32)
    sea_ref[...] = sea
    points = SUBS * cols
    line = lax.broadcasted_iota(jnp.int32, (points, LANES), 0)
    lane = lax.broadcasted_iota(jnp.int32, (points, LANES), 1)
    spread = jnp.concatenate([jnp.broadcast_to(sea[r : r + 1], (cols, LANES)) for r in range(SUBS)], axis=0)
    start = column_block(me, wide) * cols
    mine = jnp.sum(jnp.where(lane == line % cols + start, spread, 0.0), axis=1, keepdims=True)
    block_ref[...] = jnp.broadcast_to(mine, (points, LANES))

    courant = as_column(courant_ref[...])
    cosine_of = as_column(table_ref[0:1, :])
    sine_of = as_column(table_ref[1:2, :])
    bands = lax.broadcasted_iota(jnp.int32, courant.shape, 0)
    headings = lax.broadcasted_iota(jnp.int32, cosine_of.shape, 0)
    lanes = lax.broadcasted_iota(jnp.int32, (slots, LANES), 1)
    nth = lax.broadcasted_iota(jnp.int32, (slots, LANES), 0) + me * slots
    own = [jnp.zeros((slots, LANES), jnp.float32) for _ in range(2)]

    def speeds(component):
        band = component // ND
        heading = component - band * ND
        speed = jnp.sum(jnp.where(bands == band, courant, 0.0), axis=0, keepdims=True)
        cosine = jnp.sum(jnp.where(headings == heading, cosine_of, 0.0), axis=0, keepdims=True)
        sine = jnp.sum(jnp.where(headings == heading, sine_of, 0.0), axis=0, keepdims=True)
        return speed * cosine, speed * sine

    row = lax.broadcasted_iota(jnp.int32, (1, LANES), 1)
    for k in range(owner_ref.shape[0]):
        for n, share in enumerate(shares(*speeds(row + k * LANES))):
            share_ref[n : n + 1, k * LANES : (k + 1) * LANES] = share
        here = lanes + k * LANES == nth
        own = [value + jnp.where(here, one, 0.0) for value, one in zip(own, speeds(owner_ref[k : k + 1, :]))]
    east, north = (jnp.sum(value, axis=1, keepdims=True) for value in own)
    for n, share in enumerate(shares(east, north)):
        own_ref[n] = jnp.broadcast_to(share, (slots, LANES))

    for copy in large:
        copy.wait()
    head = rows_ref[0] * sea[0:1]
    tail = rows_ref[SUBS - 1] * sea[SUBS - 1 : SUBS]
    a_ref[...] = jnp.where(even, tail, head)
    b_ref[...] = jnp.where(even, head, tail)


def by_device(parts, me):
    bit = 1
    while bit < len(parts):
        flip = (me & bit) != 0
        parts = [jnp.where(flip, parts[k ^ bit], parts[k]) for k in range(len(parts))]
        bit *= 2
    return parts


def spread_kernel(ring, cols, x_ref, sea_ref, own_ref, out_ref):
    slots = x_ref.shape[1]
    sea = [jnp.broadcast_to(sea_ref[r : r + 1, :], (SUBS, LANES)) for r in range(SUBS)]
    for base in range(0, slots, SUBS):
        here = slice(base, base + SUBS)
        remain, west_in, east_in, south_in, north_in = (own_ref[k, here, :] for k in range(5))
        rows = [x_ref[r, here, :] * sea[r] for r in range(SUBS)]
        moved = []
        for r in range(SUBS):
            value = remain * rows[r] + west_in * pltpu.roll(rows[r], 1, 1)
            value = value + east_in * pltpu.roll(rows[r], LANES - 1, 1)
            if r > 0:
                value = value + south_in * rows[r - 1]
            if r < SUBS - 1:
                value = value + north_in * rows[r + 1]
            moved.append(value)
        for device, block in zip(ring, swap_lane_blocks(moved, cols)):
            out_ref[device, here, :] = block


def border_kernel(ring, cols, x_ref, a_ref, b_ref, own_ref, *outs):
    slots = x_ref.shape[1]
    me = lax.axis_index("wide")
    even = lax.axis_index("slab") % 2 == 0
    lane = lax.broadcasted_iota(jnp.int32, (SUBS, LANES), 1)
    border = (lane < cols) | (lane >= LANES - cols)
    for base in range(0, slots, SUBS):
        here = slice(base, base + SUBS)
        a, b = a_ref[here, :], b_ref[here, :]
        south = own_ref[3, here, :] * jnp.where(even, b, a)
        north = pltpu.roll(own_ref[4, here, :] * jnp.where(even, a, b), LANES - cols, 1)
        blocks = [None] * len(ring)
        for n, device in enumerate(ring):
            both = jnp.where(lane // cols == n, south, north)
            both = pltpu.roll(both, LANES - n * cols, 1) if n else both
            blocks[device] = x_ref[device, here, :] + jnp.where(border, both, 0.0)
        blocks = by_device(blocks, me)
        for k, out in zip((0,) + SWAP_ORDER, outs):
            out[here, :] = blocks[k]


def gather_kernel(ring, cols, *refs):
    parts, out_hbm, rows_ref, sem = refs[: len(ring)], *refs[len(ring) :]
    slots = rows_ref.shape[1]
    me = lax.axis_index("wide")
    by_swap = dict(zip((0,) + SWAP_ORDER, parts))
    third = slots // 3
    copies = []
    for base in range(0, slots, SUBS):
        here = slice(base, base + SUBS)
        blocks = by_device([by_swap[k][here, :] for k in range(len(ring))], me)
        for r, row in enumerate(swap_lane_blocks([blocks[device] for device in ring], cols)):
            rows_ref[r, here, :] = row
        if (base + SUBS) % third == 0:
            done = slice(base + SUBS - third, base + SUBS)
            for r in range(SUBS):
                copies.append(
                    pltpu.make_async_copy(rows_ref.at[r, done, :], out_hbm.at[done, r, :], sem.at[len(copies)])
                )
                copies[-1].start()
    for copy in copies:
        copy.wait()


ROWS_AT_ONCE = 16
EARLY = 5


def each_row(swaps, slots, owner_ref, load, store):
    me = lax.axis_index("wide")
    for k in swaps:
        first = (me ^ k) * slots

        def some(g, carry, k=k, first=first):
            for m in range(3):
                base = pl.multiple_of((g * 3 + m) * ROWS_AT_ONCE, ROWS_AT_ONCE)
                places = [(base + n, owner_ref[first + base + n]) for n in range(ROWS_AT_ONCE)]
                values = [load(k, *place) for place in places]
                for place, value in zip(places, values):
                    store(k, *place, value)
            return carry

        lax.fori_loop(0, slots // ROWS_AT_ONCE // 3, some, 0)


def to_smem(source, target, sem):
    copy = pltpu.make_async_copy(source, target, sem)
    copy.start()
    copy.wait()


def place_rows(swaps, parts, rows_ref, owner_ref):
    by_swap = dict(zip(swaps, parts))

    def store(k, row, component, value):
        rows_ref[pl.ds(component, 1), :] = value

    each_row(swaps, parts[0].shape[0], owner_ref, lambda k, row, _: by_swap[k][pl.ds(row, 1), :], store)


def place_kernel(owner_ref, *refs):
    parts, (rows_ref, owner_smem, sem) = refs[:EARLY], refs[EARLY:]
    to_smem(owner_ref, owner_smem, sem)
    place_rows(((0,) + SWAP_ORDER)[:EARLY], parts, rows_ref, owner_smem)


def contract(moved_ref, rounded_ref, square_ref, table_ref, sea, store):
    count = moved_ref.shape[1]
    for c, step in chunks(count, 2 * LANES):
        gain = lax.dot_general(
            rounded_ref[...],
            table_ref[c : c + step, :],
            (((1,), (1,)), ((), ())),
            preferred_element_type=jnp.float32,
        )
        loss = jnp.dot(square_ref[...], table_ref[:, c : c + step], preferred_element_type=jnp.float32)
        for n in range(0, step, LANES):
            moved = moved_ref[:, c + n : c + n + LANES]
            value = moved + time_step * (moved * gain[:, n : n + LANES] - loss[:, n : n + LANES])
            store(c + n, jnp.maximum(value, 0.0) * sea)


def first_kernel(wide, cols, held_ref, owner_ref, coupling_hbm, sea_ref, *refs):
    late = wide - EARLY
    parts, (rows_ref, table_ref, out_ref, a_ref, b_ref, c_ref, d_ref) = refs[:late], refs[late : late + 7]
    moved_ref, rounded_ref, square_ref, value_ref, owner_smem, sem = refs[late + 7 :]
    points, count = out_ref.shape
    row_even = lax.axis_index("slab") % 2 == 0
    col_even = column_block(lax.axis_index("wide"), wide) % 2 == 0
    copy = pltpu.make_async_copy(coupling_hbm, table_ref, sem.at[0])
    copy.start()
    to_smem(owner_ref, owner_smem, sem.at[1])
    place_rows(SWAP_ORDER[EARLY - 1 :], parts, rows_ref, owner_smem)
    for c in range(0, count, LANES):
        there = slice(c, c + LANES)
        moved = rows_ref[there, :].T
        moved_ref[:, there] = moved
        rounded_ref[:, there] = moved.astype(jnp.bfloat16)
        square_ref[:, there] = (moved * moved).astype(jnp.bfloat16)
    copy.wait()

    def store(c, value):
        there = slice(c, c + LANES)
        out_ref[:, there] = value
        head, tail = value[:cols], value[points - cols :]
        a_ref[:, there] = jnp.where(row_even, tail, head)
        b_ref[:, there] = jnp.where(row_even, head, tail)
        value_ref[...] = value
        west = value_ref[pl.ds(0, points // cols, stride=cols), :]
        east = value_ref[pl.ds(cols - 1, points // cols, stride=cols), :]
        c_ref[:, there] = jnp.where(col_even, east, west)
        d_ref[:, there] = jnp.where(col_even, west, east)

    contract(moved_ref, rounded_ref, square_ref, table_ref, sea_ref[...], store)


def second_kernel(wide, cols, x_ref, a_ref, b_ref, c_ref, d_ref, share_ref, table_ref, sea_ref, owner_ref, *refs):
    outs, (moved_ref, rounded_ref, square_ref, value_ref, owner_smem, sem) = refs[:wide], refs[wide:]
    copy = pltpu.make_async_copy(owner_ref, owner_smem, sem)
    copy.start()
    points, count = x_ref.shape
    row_even = lax.axis_index("slab") % 2 == 0
    col_even = column_block(lax.axis_index("wide"), wide) % 2 == 0
    line = lax.broadcasted_iota(jnp.int32, (points, LANES), 0) % cols
    for c in range(0, count, LANES):
        there = slice(c, c + LANES)
        here = x_ref[:, there]
        share = [share_ref[k : k + 1, there] for k in range(5)]
        a, b, side_c, side_d = a_ref[:, there], b_ref[:, there], c_ref[:, there], d_ref[:, there]

        def along(edge):
            return jnp.concatenate(
                [jnp.broadcast_to(edge[r : r + 1], (cols, LANES)) for r in range(points // cols)], axis=0
            )

        west_edge = along(jnp.where(col_even, side_d, side_c))
        east_edge = along(jnp.where(col_even, side_c, side_d))
        west = jnp.where(line == 0, west_edge, pltpu.roll(here, 1, 0))
        east = jnp.where(line == cols - 1, east_edge, pltpu.roll(here, points - 1, 0))
        south = jnp.concatenate([jnp.where(row_even, b, a), here[: points - cols]], axis=0)
        north = jnp.concatenate([here[cols:], jnp.where(row_even, a, b)], axis=0)
        moved = share[0] * here + share[1] * west
        moved = moved + share[2] * east
        moved = moved + share[3] * south
        moved = moved + share[4] * north
        moved_ref[:, there] = moved
        rounded_ref[:, there] = moved.astype(jnp.bfloat16)
        square_ref[:, there] = (moved * moved).astype(jnp.bfloat16)

    def store(c, value):
        value_ref[c : c + LANES, :] = value.T

    contract(moved_ref, rounded_ref, square_ref, table_ref, sea_ref[...], store)
    by_swap = dict(zip((0,) + SWAP_ORDER, outs))

    def put(k, row, component, value):
        by_swap[k][pl.ds(row, 1), :] = value

    copy.wait()
    each_row(
        (0,) + SWAP_ORDER, count // wide, owner_smem, lambda k, _, component: value_ref[pl.ds(component, 1), :], put
    )


def block_body(spectrum, sea_mask, courant, slot_owner, coupling):
    slots, rows, lons = spectrum.shape
    wide, slabs = lax.axis_size("wide"), lax.axis_size("slab")
    count = slots * wide
    cols = lons // wide
    points = rows * cols
    ring = ring_order(wide)
    vmem = pl.BlockSpec(memory_space=pltpu.VMEM)
    in_hbm = pl.BlockSpec(memory_space=pltpu.HBM)
    f32, bf16 = jnp.float32, jnp.bfloat16
    shape = jax.ShapeDtypeStruct

    def call(kernel, name, outs, ins, scratch=(), flops=0, on_chip_result=True, aliases={}):
        made = pl.pallas_call(
            kernel,
            out_shape=jax.tree.map(lambda out: pltpu.VMEM(out.shape, out.dtype), outs) if on_chip_result else outs,
            in_specs=ins,
            out_specs=jax.tree.map(lambda _: vmem if on_chip_result else in_hbm, outs),
            scratch_shapes=scratch,
            input_output_aliases=aliases,
            compiler_params=pltpu.CompilerParams(vmem_limit_bytes=24 << 20),
            cost_estimate=pl.CostEstimate(flops=flops, transcendentals=0, bytes_accessed=0),
            name=name,
        )

        def on_chip(*given):
            return made(
                *(
                    pltpu.with_memory_space_constraint(one, spec.memory_space)
                    for one, spec in zip(given, ins)
                )
            )

        return on_chip

    owners = slot_owner.reshape(count // LANES, LANES)
    edge = shape((slots, LANES), f32)
    trig = trig_table()
    send_a, send_b, lines, sea, sea_block, share, own = call(
        functools.partial(prepare_kernel, wide, cols),
        "prepare",
        (
            edge,
            edge,
            shape((rows, slots, LANES), f32),
            shape((rows, LANES), f32),
            shape((points, LANES), f32),
            shape((SUBS, count), f32),
            shape((5, slots, LANES), f32),
        ),
        [in_hbm] * 5,
        (
            pltpu.VMEM(sea_mask.shape, jnp.int32),
            pltpu.VMEM(owners.shape, jnp.int32),
            pltpu.VMEM((1,) + courant.shape, f32),
            pltpu.VMEM(trig.shape, f32),
            pltpu.SemaphoreType.DMA((rows,)),
            pltpu.SemaphoreType.DMA((4,)),
        ),
    )(spectrum, sea_mask, owners, courant[None, :], jnp.asarray(trig))

    def swap_rows(a, b):
        return lax.ppermute(a, "slab", pairs(slabs, 0)), lax.ppermute(b, "slab", pairs(slabs, 1))

    def swap_cols(c, d):
        def along(odd):
            return [(ring[i], ring[j]) for i, j in pairs(wide, odd, closed=True)]

        return lax.ppermute(c, "wide", along(0)), lax.ppermute(d, "wide", along(1))

    def swap_blocks(blocks):
        swaps = [
            lax.ppermute(block, "wide", [(w, w ^ k) for w in range(wide)])
            for k, block in zip(SWAP_ORDER, blocks[1:])
        ]
        return [blocks[0]] + swaps

    near = swap_rows(send_a, send_b)
    inner = call(
        functools.partial(spread_kernel, ring, cols), "spread", shape((wide, slots, LANES), f32), [vmem] * 3, flops=10**9
    )(lines, sea, own)
    blocks = call(functools.partial(border_kernel, ring, cols), "border", (edge,) * wide, [vmem] * 4)(
        inner, *near, own
    )
    scratch = (
        pltpu.VMEM((points, count), f32),
        pltpu.VMEM((points, count), bf16),
        pltpu.VMEM((points, count), bf16),
    )
    smem_owners = pltpu.SMEM(slot_owner.shape, jnp.int32)
    arrived = swap_blocks(blocks)
    held = call(
        place_kernel,
        "place",
        shape((count, points), f32),
        [in_hbm] + [vmem] * EARLY,
        (smem_owners, pltpu.SemaphoreType.DMA(())),
        flops=10**9,
    )(slot_owner, *arrived[:EARLY])
    held, table, energy, send_a, send_b, send_c, send_d = call(
        functools.partial(first_kernel, wide, cols),
        "first",
        (shape((count, points), f32), shape((count, count), bf16), shape((points, count), f32))
        + (shape((cols, count), f32),) * 2
        + (shape((rows, count), f32),) * 2,
        [vmem, in_hbm, in_hbm] + [vmem] * (1 + wide - EARLY),
        scratch + (pltpu.VMEM((points, LANES), f32), smem_owners, pltpu.SemaphoreType.DMA((2,))),
        flops=4 * points * count**2,
        aliases={0: 0},
    )(held, slot_owner, coupling, sea_block, *arrived[EARLY:])
    halos = swap_rows(send_a, send_b) + swap_cols(send_c, send_d)
    updated = call(
        functools.partial(second_kernel, wide, cols),
        "second",
        (edge,) * wide,
        [vmem] * 8 + [in_hbm],
        scratch + (pltpu.VMEM((count, points), f32), smem_owners, pltpu.SemaphoreType.DMA(())),
        flops=4 * points * count**2,
    )(energy, *halos, share, table, sea_block, slot_owner)
    return call(
        functools.partial(gather_kernel, ring, cols),
        "gather",
        shape((slots, rows, lons), f32),
        [vmem] * wide,
        (pltpu.VMEM((rows, slots, LANES), f32), pltpu.SemaphoreType.DMA((3 * rows,))),
        on_chip_result=False,
    )(*swap_blocks(updated))


def solution(mesh):
    wide, slabs = mesh.shape["wide"], mesh.shape["slab"]

    def body(spectrum, *rest):
        slots, rows, lons = spectrum.shape
        fits = rows == SUBS and lons == LANES and wide == SUBS and slots % (3 * ROWS_AT_ONCE) == 0
        fits = fits and (slots * wide) % LANES == 0
        return (block_body if fits else general_body)(spectrum, *rest)

    return jax.shard_map(
        body,
        mesh=mesh,
        in_specs=(P("wide", "slab", None), P("slab", None), P(), P(), P()),
        out_specs=P("wide", "slab", None),
        check_vma=False,
    )
```

```python
import functools
import math

import jax
import jax.numpy as jnp
import numpy as np
from jax import lax
from jax.experimental import pallas as pl
from jax.experimental.pallas import tpu as pltpu
from jax.sharding import PartitionSpec as P


ND = 36
STEPS = 2
LANES = 128
SUBS = 8
SWAP_ORDER = (4, 1, 6, 2, 5, 3, 7)

time_step = 0.5


def extended(cells, sides, width):
    for axis, dim in sides:
        count = lax.axis_size(axis)
        ends = count - 1
        head = lax.slice_in_dim(cells, 0, width, axis=dim)
        tail = lax.slice_in_dim(cells, cells.shape[dim] - width, cells.shape[dim], axis=dim)
        cells = jnp.concatenate(
            [
                lax.ppermute(tail, axis, [(i, (i + 1) % count) for i in range(ends)]),
                cells,
                lax.ppermute(head, axis, [((i + 1) % count, i) for i in range(ends)]),
            ],
            axis=dim,
        )
    return cells


def velocities(slot_owner, courant):
    band_count = courant.shape[0]
    heading = slot_owner % ND
    freq_band = slot_owner // ND
    picked = freq_band[:, None] == jnp.arange(band_count, dtype=jnp.int32)[None, :]
    wave_speed = jnp.sum(jnp.where(picked, courant[None, :], 0.0), axis=1)
    wave_angle = heading.astype(jnp.float32) * (2.0 * math.pi / ND)
    return (wave_speed * jnp.cos(wave_angle), wave_speed * jnp.sin(wave_angle))


def combine_sides(energy, west_side, east_side, south_side, north_side, east_speed, north_speed):
    east_speed = east_speed[:, None, None]
    north_speed = north_speed[:, None, None]
    remain = 1.0 - jnp.abs(east_speed) - jnp.abs(north_speed)
    result = remain * energy + jnp.maximum(east_speed, 0.0) * west_side
    result = result + jnp.maximum(-east_speed, 0.0) * east_side
    result = result + jnp.maximum(north_speed, 0.0) * south_side
    return result + jnp.maximum(-north_speed, 0.0) * north_side


def advect(energy, padded, east_speed, north_speed):
    west_side = jnp.roll(energy, 1, axis=2)
    east_side = jnp.roll(energy, -1, axis=2)
    return combine_sides(
        energy, west_side, east_side, padded[:, :-2, :], padded[:, 2:, :], east_speed, north_speed
    )


def interact(moved, slot_table):
    slot_count = moved.shape[0]
    flattened = moved.reshape(slot_count, -1)
    rounded = flattened.astype(jnp.bfloat16)
    square = (flattened * flattened).astype(jnp.bfloat16)
    gain_term = flattened * jnp.dot(slot_table, rounded, preferred_element_type=jnp.float32)
    loss_term = lax.dot_general(
        slot_table, square, (((0,), (0,)), ((), ())), preferred_element_type=jnp.float32
    )
    updated = jnp.maximum(flattened + time_step * (gain_term - loss_term), 0.0)
    return updated.reshape(moved.shape)


def general_body(spectrum, sea_mask, courant, slot_owner, coupling):
    slot_count = spectrum.shape[0]
    wide_index = lax.axis_index("wide")
    sea_float = sea_mask.astype(jnp.float32)
    slot_table = jnp.take(jnp.take(coupling, slot_owner, axis=0), slot_owner, axis=1)
    energy = spectrum * sea_float[None]
    own_slots = lax.dynamic_slice_in_dim(slot_owner, wide_index * slot_count, slot_count, 0)
    east_speed, north_speed = velocities(own_slots, courant)
    for _ in range(STEPS):
        padded = extended(energy, (("slab", 1),), 1)
        moved = advect(energy, padded, east_speed, north_speed)
        energy = (
            lax.all_to_all(
                interact(
                    lax.all_to_all(moved, "wide", split_axis=1, concat_axis=0, tiled=True),
                    slot_table,
                ),
                "wide",
                split_axis=0,
                concat_axis=1,
                tiled=True,
            )
            * sea_float[None]
        )
    return energy


def ring_order(count):
    return list(range(0, count, 2)) + list(range(1, count, 2))[::-1]


def column_block(device, count):
    half = device // 2
    return jnp.where(device % 2 == 0, half, count - 1 - half)


def trig_table():
    angle = np.arange(ND, dtype=np.float32) * np.float32(2.0 * math.pi / ND)
    table = np.zeros((SUBS, LANES), np.float32)
    table[0, :ND], table[1, :ND] = np.cos(angle), np.sin(angle)
    return table[:2]


def pairs(count, odd, closed=False):
    found = [(i, (i + 1) % count) for i in range(odd, count, 2) if closed or i + 1 < count]
    return found + [(b, a) for a, b in found]


def shares(east, north):
    return (
        1.0 - jnp.abs(east) - jnp.abs(north),
        jnp.maximum(east, 0.0),
        jnp.maximum(-east, 0.0),
        jnp.maximum(north, 0.0),
        jnp.maximum(-north, 0.0),
    )


def swap_lane_blocks(parts, width):
    count = len(parts)
    lane = lax.broadcasted_iota(jnp.int32, parts[0].shape, 1)
    bit = 1
    while bit < count:
        low = (lane & (bit * width)) == 0
        other = lane ^ (bit * width)
        done = list(parts)
        for a in range(count):
            if a & bit:
                continue
            b = a | bit
            crossed = jnp.take_along_axis(jnp.where(low, parts[b], parts[a]), other, axis=1)
            done[a] = jnp.where(low, parts[a], crossed)
            done[b] = jnp.where(low, crossed, parts[b])
        parts = done
        bit *= 2
    return parts


def chunks(count, step):
    return [(c, min(step, count - c)) for c in range(0, count, step)]


def as_column(row):
    size = row.shape[1]
    line = lax.broadcasted_iota(jnp.int32, (size, size), 0)
    lane = lax.broadcasted_iota(jnp.int32, (size, size), 1)
    column = jnp.sum(jnp.where(line == lane, row, 0.0), axis=1, keepdims=True)
    return jnp.broadcast_to(column, (size, LANES))


def speed_lookup(courant, table):
    courant = as_column(courant)
    cosine_of = as_column(table[0:1])
    sine_of = as_column(table[1:2])
    bands = lax.broadcasted_iota(jnp.int32, courant.shape, 0)
    headings = lax.broadcasted_iota(jnp.int32, cosine_of.shape, 0)

    def speeds(component):
        band = component // ND
        heading = component - band * ND
        speed = jnp.sum(jnp.where(bands == band, courant, 0.0), axis=0, keepdims=True)
        cosine = jnp.sum(jnp.where(headings == heading, cosine_of, 0.0), axis=0, keepdims=True)
        sine = jnp.sum(jnp.where(headings == heading, sine_of, 0.0), axis=0, keepdims=True)
        return speed * cosine, speed * sine

    return speeds


def prepare_kernel(x_hbm, mask_hbm, owner_hbm, courant_hbm, table_hbm, a_ref, b_ref, rows_ref, sea_ref, own_ref, mask_ref, owner_ref, courant_ref, table_ref, row_sem, sem):
    slots = a_ref.shape[0]
    me = lax.axis_index("wide")
    even = lax.axis_index("slab") % 2 == 0
    small = [
        pltpu.make_async_copy(source, target, sem.at[k])
        for k, (source, target) in enumerate(
            ((mask_hbm, mask_ref), (owner_hbm, owner_ref), (courant_hbm, courant_ref), (table_hbm, table_ref))
        )
    ]
    order = (0, SUBS - 1) + tuple(range(1, SUBS - 1))
    large = [
        pltpu.make_async_copy(x_hbm.at[:, r, :], rows_ref.at[r, pl.ds(0, slots), :], row_sem.at[r]) for r in order
    ]
    for copy in small + large:
        copy.start()
    for copy in small:
        copy.wait()
    sea = mask_ref[...].astype(jnp.float32)
    sea_ref[...] = sea
    speeds = speed_lookup(courant_ref[...], table_ref[...])
    lanes = lax.broadcasted_iota(jnp.int32, (slots, LANES), 1)
    nth = lax.broadcasted_iota(jnp.int32, (slots, LANES), 0) + me * slots
    own = [jnp.zeros((slots, LANES), jnp.float32) for _ in range(2)]

    for k in range(owner_ref.shape[0]):
        here = lanes + k * LANES == nth
        own = [value + jnp.where(here, one, 0.0) for value, one in zip(own, speeds(owner_ref[k : k + 1, :]))]
    east, north = (jnp.sum(value, axis=1, keepdims=True) for value in own)
    for n, share in enumerate(shares(east, north)):
        own_ref[n, :slots, :] = jnp.broadcast_to(share, (slots, LANES))

    for copy in large:
        copy.wait()
    head = rows_ref[0, :slots, :] * sea[0:1]
    tail = rows_ref[SUBS - 1, :slots, :] * sea[SUBS - 1 : SUBS]
    a_ref[...] = jnp.where(even, tail, head)
    b_ref[...] = jnp.where(even, head, tail)


def by_device(parts, me):
    bit = 1
    while bit < len(parts):
        flip = (me & bit) != 0
        parts = [jnp.where(flip, parts[k ^ bit], parts[k]) for k in range(len(parts))]
        bit *= 2
    return parts


def spread_kernel(ring, cols, x_ref, sea_ref, own_ref, out_ref):
    slots = x_ref.shape[1] - SUBS
    sea = [jnp.broadcast_to(sea_ref[r : r + 1, :], (SUBS, LANES)) for r in range(SUBS)]
    for base in range(0, slots, SUBS):
        here = slice(base, base + SUBS)
        remain, west_in, east_in, south_in, north_in = (own_ref[k, here, :] for k in range(5))
        rows = [x_ref[r, here, :] * sea[r] for r in range(SUBS)]
        moved = []
        for r in range(SUBS):
            value = remain * rows[r] + west_in * pltpu.roll(rows[r], 1, 1)
            value = value + east_in * pltpu.roll(rows[r], LANES - 1, 1)
            if r > 0:
                value = value + south_in * rows[r - 1]
            if r < SUBS - 1:
                value = value + north_in * rows[r + 1]
            moved.append(value)
        for device, block in zip(ring, swap_lane_blocks(moved, cols)):
            out_ref[device, here, :] = block


def border_kernel(ring, cols, x_ref, a_ref, b_ref, own_ref, *outs):
    slots = a_ref.shape[0]
    me = lax.axis_index("wide")
    even = lax.axis_index("slab") % 2 == 0
    lane = lax.broadcasted_iota(jnp.int32, (SUBS, LANES), 1)
    border = (lane < cols) | (lane >= LANES - cols)
    for base in range(0, slots, SUBS):
        here = slice(base, base + SUBS)
        a, b = a_ref[here, :], b_ref[here, :]
        south = own_ref[3, here, :] * jnp.where(even, b, a)
        north = pltpu.roll(own_ref[4, here, :] * jnp.where(even, a, b), LANES - cols, 1)
        blocks = [None] * len(ring)
        for n, device in enumerate(ring):
            both = jnp.where(lane // cols == n, south, north)
            both = pltpu.roll(both, LANES - n * cols, 1) if n else both
            blocks[device] = x_ref[device, here, :] + jnp.where(border, both, 0.0)
        blocks = by_device(blocks, me)
        for k, out in zip((0,) + SWAP_ORDER, outs):
            out[here, :] = blocks[k]


def gather_kernel(ring, cols, *refs):
    parts, out_hbm, rows_ref, sem = refs[: len(ring)], *refs[len(ring) :]
    slots = parts[0].shape[0]
    me = lax.axis_index("wide")
    by_swap = dict(zip((0,) + SWAP_ORDER, parts))
    third = slots // 3
    copies = []
    for base in range(0, slots, SUBS):
        here = slice(base, base + SUBS)
        blocks = by_device([by_swap[k][here, :] for k in range(len(ring))], me)
        for r, row in enumerate(swap_lane_blocks([blocks[device] for device in ring], cols)):
            rows_ref[r, here, :] = row
        if (base + SUBS) % third == 0:
            done = slice(base + SUBS - third, base + SUBS)
            for r in range(SUBS):
                copies.append(
                    pltpu.make_async_copy(rows_ref.at[r, done, :], out_hbm.at[done, r, :], sem.at[len(copies)])
                )
                copies[-1].start()
    for copy in copies:
        copy.wait()


ROWS_AT_ONCE = 16
EARLY = 5
LATE = 2


def each_row(swaps, slots, owner_ref, load, store):
    me = lax.axis_index("wide")
    for k in swaps:
        first = (me ^ k) * slots

        def some(g, carry, k=k, first=first):
            for m in range(3):
                base = pl.multiple_of((g * 3 + m) * ROWS_AT_ONCE, ROWS_AT_ONCE)
                places = [(base + n, owner_ref[first + base + n]) for n in range(ROWS_AT_ONCE)]
                values = [load(k, *place) for place in places]
                for place, value in zip(places, values):
                    store(k, *place, value)
            return carry

        lax.fori_loop(0, slots // ROWS_AT_ONCE // 3, some, 0)


def to_smem(source, target, sem):
    copy = pltpu.make_async_copy(source, target, sem)
    copy.start()
    copy.wait()


def place_rows(swaps, parts, rows_ref, owner_ref):
    by_swap = dict(zip(swaps, parts))

    def store(k, row, component, value):
        rows_ref[pl.ds(component, 1), :] = value

    each_row(swaps, parts[0].shape[0], owner_ref, lambda k, row, _: by_swap[k][pl.ds(row, 1), :], store)


def place_kernel(wide, cols, owner_hbm, courant_hbm, table_hbm, coupling_hbm, sea_ref, *refs):
    parts, (rows_ref, block_ref, coupling_ref, share_ref, owner_ref, courant_ref, table_ref, sem) = refs[:EARLY], refs[EARLY:]
    copies = [
        pltpu.make_async_copy(source, target, sem.at[k])
        for k, (source, target) in enumerate(
            (
                (owner_hbm, owner_ref),
                (courant_hbm, courant_ref),
                (table_hbm, table_ref),
                (coupling_hbm, coupling_ref),
            )
        )
    ]
    for copy in copies:
        copy.start()
    me = lax.axis_index("wide")
    sea = sea_ref[...]
    points = SUBS * cols
    line = lax.broadcasted_iota(jnp.int32, (points, LANES), 0)
    lane = lax.broadcasted_iota(jnp.int32, (points, LANES), 1)
    spread = jnp.concatenate([jnp.broadcast_to(sea[r : r + 1], (cols, LANES)) for r in range(SUBS)], axis=0)
    start = column_block(me, wide) * cols
    mine = jnp.sum(jnp.where(lane == line % cols + start, spread, 0.0), axis=1, keepdims=True)
    block_ref[...] = jnp.broadcast_to(mine, (points, LANES))
    for copy in copies[:-1]:
        copy.wait()
    place_rows(((0,) + SWAP_ORDER)[:EARLY], parts, rows_ref, owner_ref)
    speeds = speed_lookup(courant_ref[...], table_ref[...])
    row = lax.broadcasted_iota(jnp.int32, (1, LANES), 1)
    for c in range(0, share_ref.shape[1], LANES):
        for n, share in enumerate(shares(*speeds(row + c))):
            share_ref[n : n + 1, c : c + LANES] = share
    copies[-1].wait()


def place_more_kernel(held_ref, owner_hbm, *refs):
    parts, (rows_ref, owner_ref, sem) = refs[:LATE], refs[LATE:]
    to_smem(owner_hbm, owner_ref, sem)
    place_rows(SWAP_ORDER[EARLY - 1 : EARLY - 1 + LATE], parts, rows_ref, owner_ref)


def contract(moved_ref, rounded_ref, square_ref, table_ref, sea, store):
    count = moved_ref.shape[1]
    for c, step in chunks(count, 2 * LANES):
        gain = lax.dot_general(
            rounded_ref[...],
            table_ref[c : c + step, :],
            (((1,), (1,)), ((), ())),
            preferred_element_type=jnp.float32,
        )
        loss = jnp.dot(square_ref[...], table_ref[:, c : c + step], preferred_element_type=jnp.float32)
        for n in range(0, step, LANES):
            moved = moved_ref[:, c + n : c + n + LANES]
            value = moved + time_step * (moved * gain[:, n : n + LANES] - loss[:, n : n + LANES])
            store(c + n, jnp.maximum(value, 0.0) * sea)


def first_kernel(wide, cols, held_ref, owner_ref, table_ref, sea_ref, *refs):
    late = wide - EARLY - LATE
    parts, (rows_ref, out_ref, a_ref, b_ref, c_ref, d_ref) = refs[:late], refs[late : late + 6]
    moved_ref, rounded_ref, square_ref, value_ref, owner_smem, sem = refs[late + 6 :]
    points, count = out_ref.shape
    row_even = lax.axis_index("slab") % 2 == 0
    col_even = column_block(lax.axis_index("wide"), wide) % 2 == 0
    to_smem(owner_ref, owner_smem, sem)
    place_rows(SWAP_ORDER[EARLY + LATE - 1 :], parts, rows_ref, owner_smem)
    for c in range(0, count, LANES):
        there = slice(c, c + LANES)
        moved = rows_ref[there, :].T
        moved_ref[:, there] = moved
        rounded_ref[:, there] = moved.astype(jnp.bfloat16)
        square_ref[:, there] = (moved * moved).astype(jnp.bfloat16)

    def store(c, value):
        there = slice(c, c + LANES)
        out_ref[:, there] = value
        head, tail = value[:cols], value[points - cols :]
        a_ref[:, there] = jnp.where(row_even, tail, head)
        b_ref[:, there] = jnp.where(row_even, head, tail)
        value_ref[...] = value
        west = value_ref[pl.ds(0, points // cols, stride=cols), :]
        east = value_ref[pl.ds(cols - 1, points // cols, stride=cols), :]
        c_ref[:, there] = jnp.where(col_even, east, west)
        d_ref[:, there] = jnp.where(col_even, west, east)

    contract(moved_ref, rounded_ref, square_ref, table_ref, sea_ref[...], store)


def second_kernel(wide, cols, x_ref, a_ref, b_ref, c_ref, d_ref, share_ref, table_ref, sea_ref, owner_ref, *refs):
    outs, (moved_ref, rounded_ref, square_ref, value_ref, owner_smem, sem) = refs[:wide], refs[wide:]
    copy = pltpu.make_async_copy(owner_ref, owner_smem, sem)
    copy.start()
    points, count = x_ref.shape
    row_even = lax.axis_index("slab") % 2 == 0
    col_even = column_block(lax.axis_index("wide"), wide) % 2 == 0
    line = lax.broadcasted_iota(jnp.int32, (points, LANES), 0) % cols
    for c in range(0, count, LANES):
        there = slice(c, c + LANES)
        here = x_ref[:, there]
        share = [share_ref[k : k + 1, there] for k in range(5)]
        a, b, side_c, side_d = a_ref[:, there], b_ref[:, there], c_ref[:, there], d_ref[:, there]

        def along(edge):
            return jnp.concatenate(
                [jnp.broadcast_to(edge[r : r + 1], (cols, LANES)) for r in range(points // cols)], axis=0
            )

        west_edge = along(jnp.where(col_even, side_d, side_c))
        east_edge = along(jnp.where(col_even, side_c, side_d))
        west = jnp.where(line == 0, west_edge, pltpu.roll(here, 1, 0))
        east = jnp.where(line == cols - 1, east_edge, pltpu.roll(here, points - 1, 0))
        south = jnp.concatenate([jnp.where(row_even, b, a), here[: points - cols]], axis=0)
        north = jnp.concatenate([here[cols:], jnp.where(row_even, a, b)], axis=0)
        moved = share[0] * here + share[1] * west
        moved = moved + share[2] * east
        moved = moved + share[3] * south
        moved = moved + share[4] * north
        moved_ref[:, there] = moved
        rounded_ref[:, there] = moved.astype(jnp.bfloat16)
        square_ref[:, there] = (moved * moved).astype(jnp.bfloat16)

    def store(c, value):
        value_ref[c : c + LANES, :] = value.T

    contract(moved_ref, rounded_ref, square_ref, table_ref, sea_ref[...], store)
    by_swap = dict(zip((0,) + SWAP_ORDER, outs))

    def put(k, row, component, value):
        by_swap[k][pl.ds(row, 1), :] = value

    copy.wait()
    each_row(
        (0,) + SWAP_ORDER, count // wide, owner_smem, lambda k, _, component: value_ref[pl.ds(component, 1), :], put
    )


def block_body(spectrum, sea_mask, courant, slot_owner, coupling):
    slots, rows, lons = spectrum.shape
    wide, slabs = lax.axis_size("wide"), lax.axis_size("slab")
    count = slots * wide
    cols = lons // wide
    points = rows * cols
    ring = ring_order(wide)
    vmem = pl.BlockSpec(memory_space=pltpu.VMEM)
    in_hbm = pl.BlockSpec(memory_space=pltpu.HBM)
    f32, bf16 = jnp.float32, jnp.bfloat16
    shape = jax.ShapeDtypeStruct

    def call(kernel, outs, ins, scratch=(), flops=0, on_chip_result=True, aliases={}):
        made = pl.pallas_call(
            kernel,
            out_shape=jax.tree.map(lambda out: pltpu.VMEM(out.shape, out.dtype), outs) if on_chip_result else outs,
            in_specs=ins,
            out_specs=jax.tree.map(lambda _: vmem if on_chip_result else in_hbm, outs),
            scratch_shapes=scratch,
            input_output_aliases=aliases,
            compiler_params=pltpu.CompilerParams(vmem_limit_bytes=24 << 20),
            cost_estimate=pl.CostEstimate(flops=flops, transcendentals=0, bytes_accessed=0),
        )

        def on_chip(*given):
            return made(
                *(
                    pltpu.with_memory_space_constraint(one, spec.memory_space)
                    for one, spec in zip(given, ins)
                )
            )

        return on_chip

    owners = slot_owner.reshape(count // LANES, LANES)
    edge = shape((slots, LANES), f32)
    trig = trig_table()
    send_a, send_b, lines, sea, own = call(
        prepare_kernel,
        (
            edge,
            edge,
            shape((rows, slots + SUBS, LANES), f32),
            shape((rows, LANES), f32),
            shape((5, slots + SUBS, LANES), f32),
        ),
        [in_hbm] * 5,
        (
            pltpu.VMEM(sea_mask.shape, jnp.int32),
            pltpu.VMEM(owners.shape, jnp.int32),
            pltpu.VMEM((1,) + courant.shape, f32),
            pltpu.VMEM(trig.shape, f32),
            pltpu.SemaphoreType.DMA((rows,)),
            pltpu.SemaphoreType.DMA((4,)),
        ),
    )(spectrum, sea_mask, owners, courant[None, :], jnp.asarray(trig))

    def swap_rows(a, b):
        return lax.ppermute(a, "slab", pairs(slabs, 0)), lax.ppermute(b, "slab", pairs(slabs, 1))

    def swap_cols(c, d):
        def along(odd):
            return [(ring[i], ring[j]) for i, j in pairs(wide, odd, closed=True)]

        return lax.ppermute(c, "wide", along(0)), lax.ppermute(d, "wide", along(1))

    def swap_blocks(blocks):
        swaps = [
            lax.ppermute(block, "wide", [(w, w ^ k) for w in range(wide)])
            for k, block in zip(SWAP_ORDER, blocks[1:])
        ]
        return [blocks[0]] + swaps

    near = swap_rows(send_a, send_b)
    inner = call(
        functools.partial(spread_kernel, ring, cols), shape((wide, slots + SUBS, LANES), f32), [vmem] * 3, flops=10**9
    )(lines, sea, own)
    blocks = call(functools.partial(border_kernel, ring, cols), (edge,) * wide, [vmem] * 4)(
        inner, *near, own
    )
    scratch = (
        pltpu.VMEM((points, count), f32),
        pltpu.VMEM((points, count), bf16),
        pltpu.VMEM((points, count), bf16),
    )
    smem_owners = pltpu.SMEM(slot_owner.shape, jnp.int32)
    arrived = swap_blocks(blocks)
    held, sea_block, table, share = call(
        functools.partial(place_kernel, wide, cols),
        (
            shape((count, points), f32),
            shape((points, LANES), f32),
            shape((count, count), bf16),
            shape((SUBS, count), f32),
        ),
        [in_hbm] * 4 + [vmem] * (1 + EARLY),
        (
            smem_owners,
            pltpu.VMEM((1,) + courant.shape, f32),
            pltpu.VMEM(trig.shape, f32),
            pltpu.SemaphoreType.DMA((4,)),
        ),
        flops=10**9,
    )(slot_owner, courant[None, :], jnp.asarray(trig), coupling, sea, *arrived[:EARLY])
    held = call(
        place_more_kernel,
        shape((count, points), f32),
        [vmem, in_hbm] + [vmem] * LATE,
        (smem_owners, pltpu.SemaphoreType.DMA(())),
        flops=10**9,
        aliases={0: 0},
    )(held, slot_owner, *arrived[EARLY : EARLY + LATE])
    held, energy, send_a, send_b, send_c, send_d = call(
        functools.partial(first_kernel, wide, cols),
        (shape((count, points), f32),)
        + (shape((points, count), f32),)
        + (shape((cols, count), f32),) * 2
        + (shape((rows, count), f32),) * 2,
        [vmem, in_hbm, vmem] + [vmem] * (1 + wide - EARLY - LATE),
        scratch + (pltpu.VMEM((points, LANES), f32), smem_owners, pltpu.SemaphoreType.DMA(())),
        flops=4 * points * count**2,
        aliases={0: 0},
    )(held, slot_owner, table, sea_block, *arrived[EARLY + LATE :])
    sides = swap_cols(send_c, send_d)
    halos = swap_rows(send_a, send_b) + sides
    updated = call(
        functools.partial(second_kernel, wide, cols),
        (edge,) * wide,
        [vmem] * 8 + [in_hbm],
        scratch + (pltpu.VMEM((count, points), f32), smem_owners, pltpu.SemaphoreType.DMA(())),
        flops=4 * points * count**2,
    )(energy, *halos, share, table, sea_block, slot_owner)
    return call(
        functools.partial(gather_kernel, ring, cols),
        shape((slots, rows, lons), f32),
        [vmem] * wide,
        (pltpu.VMEM((rows, slots + SUBS, LANES), f32), pltpu.SemaphoreType.DMA((3 * rows,))),
        on_chip_result=False,
    )(*swap_blocks(updated))


def solution(mesh):
    wide = mesh.shape["wide"]

    def body(spectrum, *rest):
        slots, rows, lons = spectrum.shape
        fits = rows == SUBS and lons == LANES and wide == SUBS and slots % (3 * ROWS_AT_ONCE) == 0
        fits = fits and (slots * wide) % LANES == 0
        return (block_body if fits else general_body)(spectrum, *rest)

    return jax.shard_map(
        body,
        mesh=mesh,
        in_specs=(P("wide", "slab", None), P("slab", None), P(), P(), P()),
        out_specs=P("wide", "slab", None),
        check_vma=False,
    )
```

```python
import functools
import math

import jax
import jax.numpy as jnp
import numpy as np
from jax import lax
from jax.experimental import pallas as pl
from jax.experimental.pallas import tpu as pltpu
from jax.sharding import PartitionSpec as P


ND = 36
STEPS = 2
LANES = 128
SUBS = 8
SWAP_ORDER = (4, 1, 6, 2, 5, 3, 7)

time_step = 0.5


def extended(cells, sides, width):
    for axis, dim in sides:
        count = lax.axis_size(axis)
        ends = count - 1
        head = lax.slice_in_dim(cells, 0, width, axis=dim)
        tail = lax.slice_in_dim(cells, cells.shape[dim] - width, cells.shape[dim], axis=dim)
        cells = jnp.concatenate(
            [
                lax.ppermute(tail, axis, [(i, (i + 1) % count) for i in range(ends)]),
                cells,
                lax.ppermute(head, axis, [((i + 1) % count, i) for i in range(ends)]),
            ],
            axis=dim,
        )
    return cells


def velocities(slot_owner, courant):
    band_count = courant.shape[0]
    heading = slot_owner % ND
    freq_band = slot_owner // ND
    picked = freq_band[:, None] == jnp.arange(band_count, dtype=jnp.int32)[None, :]
    wave_speed = jnp.sum(jnp.where(picked, courant[None, :], 0.0), axis=1)
    wave_angle = heading.astype(jnp.float32) * (2.0 * math.pi / ND)
    return (wave_speed * jnp.cos(wave_angle), wave_speed * jnp.sin(wave_angle))


def combine_sides(energy, west_side, east_side, south_side, north_side, east_speed, north_speed):
    east_speed = east_speed[:, None, None]
    north_speed = north_speed[:, None, None]
    remain = 1.0 - jnp.abs(east_speed) - jnp.abs(north_speed)
    result = remain * energy + jnp.maximum(east_speed, 0.0) * west_side
    result = result + jnp.maximum(-east_speed, 0.0) * east_side
    result = result + jnp.maximum(north_speed, 0.0) * south_side
    return result + jnp.maximum(-north_speed, 0.0) * north_side


def advect(energy, padded, east_speed, north_speed):
    west_side = jnp.roll(energy, 1, axis=2)
    east_side = jnp.roll(energy, -1, axis=2)
    return combine_sides(
        energy, west_side, east_side, padded[:, :-2, :], padded[:, 2:, :], east_speed, north_speed
    )


def interact(moved, slot_table):
    slot_count = moved.shape[0]
    flattened = moved.reshape(slot_count, -1)
    rounded = flattened.astype(jnp.bfloat16)
    square = (flattened * flattened).astype(jnp.bfloat16)
    gain_term = flattened * jnp.dot(slot_table, rounded, preferred_element_type=jnp.float32)
    loss_term = lax.dot_general(
        slot_table, square, (((0,), (0,)), ((), ())), preferred_element_type=jnp.float32
    )
    updated = jnp.maximum(flattened + time_step * (gain_term - loss_term), 0.0)
    return updated.reshape(moved.shape)


def general_body(spectrum, sea_mask, courant, slot_owner, coupling):
    slot_count = spectrum.shape[0]
    wide_index = lax.axis_index("wide")
    sea_float = sea_mask.astype(jnp.float32)
    slot_table = jnp.take(jnp.take(coupling, slot_owner, axis=0), slot_owner, axis=1)
    energy = spectrum * sea_float[None]
    own_slots = lax.dynamic_slice_in_dim(slot_owner, wide_index * slot_count, slot_count, 0)
    east_speed, north_speed = velocities(own_slots, courant)
    for _ in range(STEPS):
        padded = extended(energy, (("slab", 1),), 1)
        moved = advect(energy, padded, east_speed, north_speed)
        energy = (
            lax.all_to_all(
                interact(
                    lax.all_to_all(moved, "wide", split_axis=1, concat_axis=0, tiled=True),
                    slot_table,
                ),
                "wide",
                split_axis=0,
                concat_axis=1,
                tiled=True,
            )
            * sea_float[None]
        )
    return energy


def ring_order(count):
    return list(range(0, count, 2)) + list(range(1, count, 2))[::-1]


def column_block(device, count):
    half = device // 2
    return jnp.where(device % 2 == 0, half, count - 1 - half)


def trig_table():
    angle = np.arange(ND, dtype=np.float32) * np.float32(2.0 * math.pi / ND)
    table = np.zeros((SUBS, LANES), np.float32)
    table[0, :ND], table[1, :ND] = np.cos(angle), np.sin(angle)
    return table[:2]


def pairs(count, odd, closed=False):
    found = [(i, (i + 1) % count) for i in range(odd, count, 2) if closed or i + 1 < count]
    return found + [(b, a) for a, b in found]


def shares(east, north):
    return (
        1.0 - jnp.abs(east) - jnp.abs(north),
        jnp.maximum(east, 0.0),
        jnp.maximum(-east, 0.0),
        jnp.maximum(north, 0.0),
        jnp.maximum(-north, 0.0),
    )


def swap_lane_blocks(parts, width):
    count = len(parts)
    lane = lax.broadcasted_iota(jnp.int32, parts[0].shape, 1)
    bit = 1
    while bit < count:
        low = (lane & (bit * width)) == 0
        other = lane ^ (bit * width)
        done = list(parts)
        for a in range(count):
            if a & bit:
                continue
            b = a | bit
            crossed = jnp.where(low, parts[b], parts[a])
            if 2 * bit * width == LANES:
                crossed = pltpu.roll(crossed, bit * width, 1)
            else:
                crossed = jnp.take_along_axis(crossed, other, axis=1)
            done[a] = jnp.where(low, parts[a], crossed)
            done[b] = jnp.where(low, crossed, parts[b])
        parts = done
        bit *= 2
    return parts


def chunks(count, step):
    return [(c, min(step, count - c)) for c in range(0, count, step)]


def as_column(row):
    size = row.shape[1]
    line = lax.broadcasted_iota(jnp.int32, (size, size), 0)
    lane = lax.broadcasted_iota(jnp.int32, (size, size), 1)
    column = jnp.sum(jnp.where(line == lane, row, 0.0), axis=1, keepdims=True)
    return jnp.broadcast_to(column, (size, LANES))


def speed_lookup(courant, table):
    courant = as_column(courant)
    cosine_of = as_column(table[0:1])
    sine_of = as_column(table[1:2])
    bands = lax.broadcasted_iota(jnp.int32, courant.shape, 0)
    headings = lax.broadcasted_iota(jnp.int32, cosine_of.shape, 0)

    def speeds(component):
        band = component // ND
        heading = component - band * ND
        speed = jnp.sum(jnp.where(bands == band, courant, 0.0), axis=0, keepdims=True)
        cosine = jnp.sum(jnp.where(headings == heading, cosine_of, 0.0), axis=0, keepdims=True)
        sine = jnp.sum(jnp.where(headings == heading, sine_of, 0.0), axis=0, keepdims=True)
        return speed * cosine, speed * sine

    return speeds


def prepare_kernel(x_hbm, mask_hbm, owner_hbm, courant_hbm, table_hbm, a_ref, b_ref, rows_ref, sea_ref, own_ref, mask_ref, owner_ref, courant_ref, table_ref, row_sem, sem):
    slots = a_ref.shape[0]
    me = lax.axis_index("wide")
    even = lax.axis_index("slab") % 2 == 0
    small = [
        pltpu.make_async_copy(source, target, sem.at[k])
        for k, (source, target) in enumerate(
            ((mask_hbm, mask_ref), (owner_hbm, owner_ref), (courant_hbm, courant_ref), (table_hbm, table_ref))
        )
    ]
    order = (0, SUBS - 1) + tuple(range(1, SUBS - 1))
    large = [
        pltpu.make_async_copy(x_hbm.at[:, r, :], rows_ref.at[r, pl.ds(0, slots), :], row_sem.at[r]) for r in order
    ]
    for copy in small + large:
        copy.start()
    for copy in small:
        copy.wait()
    sea = mask_ref[...].astype(jnp.float32)
    sea_ref[...] = sea
    speeds = speed_lookup(courant_ref[...], table_ref[...])
    lanes = lax.broadcasted_iota(jnp.int32, (slots, LANES), 1)
    nth = lax.broadcasted_iota(jnp.int32, (slots, LANES), 0) + me * slots
    own = [jnp.zeros((slots, LANES), jnp.float32) for _ in range(2)]

    for k in range(owner_ref.shape[0]):
        here = lanes + k * LANES == nth
        own = [value + jnp.where(here, one, 0.0) for value, one in zip(own, speeds(owner_ref[k : k + 1, :]))]
    east, north = (jnp.sum(value, axis=1, keepdims=True) for value in own)
    for n, share in enumerate(shares(east, north)):
        own_ref[n, :slots, :] = jnp.broadcast_to(share, (slots, LANES))

    for copy in large:
        copy.wait()
    head = rows_ref[0, :slots, :] * sea[0:1]
    tail = rows_ref[SUBS - 1, :slots, :] * sea[SUBS - 1 : SUBS]
    a_ref[...] = jnp.where(even, tail, head)
    b_ref[...] = jnp.where(even, head, tail)


def by_device(parts, me):
    bit = 1
    while bit < len(parts):
        flip = (me & bit) != 0
        parts = [jnp.where(flip, parts[k ^ bit], parts[k]) for k in range(len(parts))]
        bit *= 2
    return parts


def spread_kernel(ring, cols, x_ref, sea_ref, own_ref, out_ref):
    slots = x_ref.shape[1] - SUBS
    sea = [jnp.broadcast_to(sea_ref[r : r + 1, :], (SUBS, LANES)) for r in range(SUBS)]
    for base in range(0, slots, SUBS):
        here = slice(base, base + SUBS)
        remain, west_in, east_in, south_in, north_in = (own_ref[k, here, :] for k in range(5))
        rows = [x_ref[r, here, :] * sea[r] for r in range(SUBS)]
        moved = []
        for r in range(SUBS):
            value = remain * rows[r] + west_in * pltpu.roll(rows[r], 1, 1)
            value = value + east_in * pltpu.roll(rows[r], LANES - 1, 1)
            if r > 0:
                value = value + south_in * rows[r - 1]
            if r < SUBS - 1:
                value = value + north_in * rows[r + 1]
            moved.append(value)
        for device, block in zip(ring, swap_lane_blocks(moved, cols)):
            out_ref[device, here, :] = block


def border_kernel(ring, cols, x_ref, a_ref, b_ref, own_ref, *outs):
    slots = a_ref.shape[0]
    me = lax.axis_index("wide")
    even = lax.axis_index("slab") % 2 == 0
    lane = lax.broadcasted_iota(jnp.int32, (SUBS, LANES), 1)
    border = (lane < cols) | (lane >= LANES - cols)
    for base in range(0, slots, SUBS):
        here = slice(base, base + SUBS)
        a, b = a_ref[here, :], b_ref[here, :]
        south = own_ref[3, here, :] * jnp.where(even, b, a)
        north = pltpu.roll(own_ref[4, here, :] * jnp.where(even, a, b), LANES - cols, 1)
        blocks = [None] * len(ring)
        for n, device in enumerate(ring):
            both = jnp.where(lane // cols == n, south, north)
            both = pltpu.roll(both, LANES - n * cols, 1) if n else both
            blocks[device] = x_ref[device, here, :] + jnp.where(border, both, 0.0)
        blocks = by_device(blocks, me)
        for k, out in zip((0,) + SWAP_ORDER, outs):
            out[here, :] = blocks[k]


def gather_kernel(ring, cols, *refs):
    parts, out_hbm, rows_ref, sem = refs[: len(ring)], *refs[len(ring) :]
    slots = parts[0].shape[0]
    me = lax.axis_index("wide")
    by_swap = dict(zip((0,) + SWAP_ORDER, parts))
    third = slots // 3
    copies = []
    for base in range(0, slots, SUBS):
        here = slice(base, base + SUBS)
        blocks = by_device([by_swap[k][here, :] for k in range(len(ring))], me)
        for r, row in enumerate(swap_lane_blocks([blocks[device] for device in ring], cols)):
            rows_ref[r, here, :] = row
        if (base + SUBS) % third == 0:
            done = slice(base + SUBS - third, base + SUBS)
            for r in range(SUBS):
                copies.append(
                    pltpu.make_async_copy(rows_ref.at[r, done, :], out_hbm.at[done, r, :], sem.at[len(copies)])
                )
                copies[-1].start()
    for copy in copies:
        copy.wait()


ROWS_AT_ONCE = 16
EARLY = 5
LATE = 2


def each_row(swaps, slots, owner_ref, load, store):
    me = lax.axis_index("wide")
    for k in swaps:
        first = (me ^ k) * slots

        def some(g, carry, k=k, first=first):
            for m in range(3):
                base = pl.multiple_of((g * 3 + m) * ROWS_AT_ONCE, ROWS_AT_ONCE)
                places = [(base + n, owner_ref[first + base + n]) for n in range(ROWS_AT_ONCE)]
                values = [load(k, *place) for place in places]
                for place, value in zip(places, values):
                    store(k, *place, value)
            return carry

        lax.fori_loop(0, slots // ROWS_AT_ONCE // 3, some, 0)


def to_smem(source, target, sem):
    copy = pltpu.make_async_copy(source, target, sem)
    copy.start()
    copy.wait()


def place_rows(swaps, parts, rows_ref, owner_ref):
    by_swap = dict(zip(swaps, parts))

    def store(k, row, component, value):
        rows_ref[pl.ds(component, 1), :] = value

    each_row(swaps, parts[0].shape[0], owner_ref, lambda k, row, _: by_swap[k][pl.ds(row, 1), :], store)


def place_kernel(wide, cols, owner_hbm, courant_hbm, table_hbm, coupling_hbm, sea_ref, *refs):
    parts, (rows_ref, block_ref, coupling_ref, share_ref, owner_ref, courant_ref, table_ref, sem) = refs[:EARLY], refs[EARLY:]
    copies = [
        pltpu.make_async_copy(source, target, sem.at[k])
        for k, (source, target) in enumerate(
            (
                (owner_hbm, owner_ref),
                (courant_hbm, courant_ref),
                (table_hbm, table_ref),
                (coupling_hbm, coupling_ref),
            )
        )
    ]
    for copy in copies:
        copy.start()
    me = lax.axis_index("wide")
    sea = sea_ref[...]
    points = SUBS * cols
    line = lax.broadcasted_iota(jnp.int32, (points, LANES), 0)
    lane = lax.broadcasted_iota(jnp.int32, (points, LANES), 1)
    spread = jnp.concatenate([jnp.broadcast_to(sea[r : r + 1], (cols, LANES)) for r in range(SUBS)], axis=0)
    start = column_block(me, wide) * cols
    mine = jnp.sum(jnp.where(lane == line % cols + start, spread, 0.0), axis=1, keepdims=True)
    block_ref[...] = jnp.broadcast_to(mine, (points, LANES))
    for copy in copies[:-1]:
        copy.wait()
    place_rows(((0,) + SWAP_ORDER)[:EARLY], parts, rows_ref, owner_ref)
    speeds = speed_lookup(courant_ref[...], table_ref[...])
    row = lax.broadcasted_iota(jnp.int32, (1, LANES), 1)
    for c in range(0, share_ref.shape[1], LANES):
        for n, share in enumerate(shares(*speeds(row + c))):
            share_ref[n : n + 1, c : c + LANES] = share
    copies[-1].wait()


def place_more_kernel(held_ref, owner_hbm, *refs):
    parts, (rows_ref, owner_ref, sem) = refs[:LATE], refs[LATE:]
    to_smem(owner_hbm, owner_ref, sem)
    place_rows(SWAP_ORDER[EARLY - 1 : EARLY - 1 + LATE], parts, rows_ref, owner_ref)


def contract(moved_ref, rounded_ref, square_ref, table_ref, sea, store):
    count = moved_ref.shape[1]
    for c, step in chunks(count, 2 * LANES):
        gain = lax.dot_general(
            rounded_ref[...],
            table_ref[c : c + step, :],
            (((1,), (1,)), ((), ())),
            preferred_element_type=jnp.float32,
        )
        loss = jnp.dot(square_ref[...], table_ref[:, c : c + step], preferred_element_type=jnp.float32)
        for n in range(0, step, LANES):
            moved = moved_ref[:, c + n : c + n + LANES]
            value = moved + time_step * (moved * gain[:, n : n + LANES] - loss[:, n : n + LANES])
            store(c + n, jnp.maximum(value, 0.0) * sea)


def first_kernel(wide, cols, held_ref, owner_ref, table_ref, sea_ref, *refs):
    late = wide - EARLY - LATE
    parts, (rows_ref, out_ref, a_ref, b_ref, c_ref, d_ref) = refs[:late], refs[late : late + 6]
    moved_ref, rounded_ref, square_ref, value_ref, owner_smem, sem = refs[late + 6 :]
    points, count = out_ref.shape
    row_even = lax.axis_index("slab") % 2 == 0
    col_even = column_block(lax.axis_index("wide"), wide) % 2 == 0
    to_smem(owner_ref, owner_smem, sem)
    place_rows(SWAP_ORDER[EARLY + LATE - 1 :], parts, rows_ref, owner_smem)
    for c in range(0, count, LANES):
        there = slice(c, c + LANES)
        moved = rows_ref[there, :].T
        moved_ref[:, there] = moved
        rounded_ref[:, there] = moved.astype(jnp.bfloat16)
        square_ref[:, there] = (moved * moved).astype(jnp.bfloat16)

    def store(c, value):
        there = slice(c, c + LANES)
        out_ref[:, there] = value
        head, tail = value[:cols], value[points - cols :]
        a_ref[:, there] = jnp.where(row_even, tail, head)
        b_ref[:, there] = jnp.where(row_even, head, tail)
        value_ref[...] = value
        west = value_ref[pl.ds(0, points // cols, stride=cols), :]
        east = value_ref[pl.ds(cols - 1, points // cols, stride=cols), :]
        c_ref[:, there] = jnp.where(col_even, east, west)
        d_ref[:, there] = jnp.where(col_even, west, east)

    contract(moved_ref, rounded_ref, square_ref, table_ref, sea_ref[...], store)


def second_kernel(wide, cols, x_ref, a_ref, b_ref, c_ref, d_ref, share_ref, table_ref, sea_ref, owner_ref, *refs):
    outs, (moved_ref, rounded_ref, square_ref, value_ref, owner_smem, sem) = refs[:wide], refs[wide:]
    copy = pltpu.make_async_copy(owner_ref, owner_smem, sem)
    copy.start()
    points, count = x_ref.shape
    row_even = lax.axis_index("slab") % 2 == 0
    col_even = column_block(lax.axis_index("wide"), wide) % 2 == 0
    line = lax.broadcasted_iota(jnp.int32, (points, LANES), 0) % cols
    for c in range(0, count, LANES):
        there = slice(c, c + LANES)
        here = x_ref[:, there]
        share = [share_ref[k : k + 1, there] for k in range(5)]
        a, b, side_c, side_d = a_ref[:, there], b_ref[:, there], c_ref[:, there], d_ref[:, there]

        def along(edge):
            return jnp.concatenate(
                [jnp.broadcast_to(edge[r : r + 1], (cols, LANES)) for r in range(points // cols)], axis=0
            )

        west_edge = along(jnp.where(col_even, side_d, side_c))
        east_edge = along(jnp.where(col_even, side_c, side_d))
        west = jnp.where(line == 0, west_edge, pltpu.roll(here, 1, 0))
        east = jnp.where(line == cols - 1, east_edge, pltpu.roll(here, points - 1, 0))
        south = jnp.concatenate([jnp.where(row_even, b, a), here[: points - cols]], axis=0)
        north = jnp.concatenate([here[cols:], jnp.where(row_even, a, b)], axis=0)
        moved = share[0] * here + share[1] * west
        moved = moved + share[2] * east
        moved = moved + share[3] * south
        moved = moved + share[4] * north
        moved_ref[:, there] = moved
        rounded_ref[:, there] = moved.astype(jnp.bfloat16)
        square_ref[:, there] = (moved * moved).astype(jnp.bfloat16)

    def store(c, value):
        value_ref[c : c + LANES, :] = value.T

    contract(moved_ref, rounded_ref, square_ref, table_ref, sea_ref[...], store)
    by_swap = dict(zip((0,) + SWAP_ORDER, outs))

    def put(k, row, component, value):
        by_swap[k][pl.ds(row, 1), :] = value

    copy.wait()
    each_row(
        (0,) + SWAP_ORDER, count // wide, owner_smem, lambda k, _, component: value_ref[pl.ds(component, 1), :], put
    )


def block_body(spectrum, sea_mask, courant, slot_owner, coupling):
    slots, rows, lons = spectrum.shape
    wide, slabs = lax.axis_size("wide"), lax.axis_size("slab")
    count = slots * wide
    cols = lons // wide
    points = rows * cols
    ring = ring_order(wide)
    vmem = pl.BlockSpec(memory_space=pltpu.VMEM)
    in_hbm = pl.BlockSpec(memory_space=pltpu.HBM)
    f32, bf16 = jnp.float32, jnp.bfloat16
    shape = jax.ShapeDtypeStruct

    def call(kernel, outs, ins, scratch=(), flops=0, on_chip_result=True, aliases={}):
        made = pl.pallas_call(
            kernel,
            out_shape=jax.tree.map(lambda out: pltpu.VMEM(out.shape, out.dtype), outs) if on_chip_result else outs,
            in_specs=ins,
            out_specs=jax.tree.map(lambda _: vmem if on_chip_result else in_hbm, outs),
            scratch_shapes=scratch,
            input_output_aliases=aliases,
            compiler_params=pltpu.CompilerParams(vmem_limit_bytes=24 << 20),
            cost_estimate=pl.CostEstimate(flops=flops, transcendentals=0, bytes_accessed=0),
        )

        def on_chip(*given):
            return made(
                *(
                    pltpu.with_memory_space_constraint(one, spec.memory_space)
                    for one, spec in zip(given, ins)
                )
            )

        return on_chip

    owners = slot_owner.reshape(count // LANES, LANES)
    edge = shape((slots, LANES), f32)
    trig = trig_table()
    send_a, send_b, lines, sea, own = call(
        prepare_kernel,
        (
            edge,
            edge,
            shape((rows, slots + SUBS, LANES), f32),
            shape((rows, LANES), f32),
            shape((5, slots + SUBS, LANES), f32),
        ),
        [in_hbm] * 5,
        (
            pltpu.VMEM(sea_mask.shape, jnp.int32),
            pltpu.VMEM(owners.shape, jnp.int32),
            pltpu.VMEM((1,) + courant.shape, f32),
            pltpu.VMEM(trig.shape, f32),
            pltpu.SemaphoreType.DMA((rows,)),
            pltpu.SemaphoreType.DMA((4,)),
        ),
    )(spectrum, sea_mask, owners, courant[None, :], jnp.asarray(trig))

    def swap_rows(a, b):
        return lax.ppermute(a, "slab", pairs(slabs, 0)), lax.ppermute(b, "slab", pairs(slabs, 1))

    def swap_cols(c, d):
        def along(odd):
            return [(ring[i], ring[j]) for i, j in pairs(wide, odd, closed=True)]

        return lax.ppermute(c, "wide", along(0)), lax.ppermute(d, "wide", along(1))

    def swap_blocks(blocks):
        swaps = [
            lax.ppermute(block, "wide", [(w, w ^ k) for w in range(wide)])
            for k, block in zip(SWAP_ORDER, blocks[1:])
        ]
        return [blocks[0]] + swaps

    near = swap_rows(send_a, send_b)
    inner = call(
        functools.partial(spread_kernel, ring, cols), shape((wide, slots + SUBS, LANES), f32), [vmem] * 3, flops=10**9
    )(lines, sea, own)
    blocks = call(functools.partial(border_kernel, ring, cols), (edge,) * wide, [vmem] * 4)(
        inner, *near, own
    )
    scratch = (
        pltpu.VMEM((points, count), f32),
        pltpu.VMEM((points, count), bf16),
        pltpu.VMEM((points, count), bf16),
    )
    smem_owners = pltpu.SMEM(slot_owner.shape, jnp.int32)
    arrived = swap_blocks(blocks)
    held, sea_block, table, share = call(
        functools.partial(place_kernel, wide, cols),
        (
            shape((count, points), f32),
            shape((points, LANES), f32),
            shape((count, count), bf16),
            shape((SUBS, count), f32),
        ),
        [in_hbm] * 4 + [vmem] * (1 + EARLY),
        (
            smem_owners,
            pltpu.VMEM((1,) + courant.shape, f32),
            pltpu.VMEM(trig.shape, f32),
            pltpu.SemaphoreType.DMA((4,)),
        ),
        flops=10**9,
    )(slot_owner, courant[None, :], jnp.asarray(trig), coupling, sea, *arrived[:EARLY])
    held = call(
        place_more_kernel,
        shape((count, points), f32),
        [vmem, in_hbm] + [vmem] * LATE,
        (smem_owners, pltpu.SemaphoreType.DMA(())),
        flops=10**9,
        aliases={0: 0},
    )(held, slot_owner, *arrived[EARLY : EARLY + LATE])
    held, energy, send_a, send_b, send_c, send_d = call(
        functools.partial(first_kernel, wide, cols),
        (shape((count, points), f32),)
        + (shape((points, count), f32),)
        + (shape((cols, count), f32),) * 2
        + (shape((rows, count), f32),) * 2,
        [vmem, in_hbm, vmem] + [vmem] * (1 + wide - EARLY - LATE),
        scratch + (pltpu.VMEM((points, LANES), f32), smem_owners, pltpu.SemaphoreType.DMA(())),
        flops=4 * points * count**2,
        aliases={0: 0},
    )(held, slot_owner, table, sea_block, *arrived[EARLY + LATE :])
    sides = swap_cols(send_c, send_d)
    halos = swap_rows(send_a, send_b) + sides
    updated = call(
        functools.partial(second_kernel, wide, cols),
        (edge,) * wide,
        [vmem] * 8 + [in_hbm],
        scratch + (pltpu.VMEM((count, points), f32), smem_owners, pltpu.SemaphoreType.DMA(())),
        flops=4 * points * count**2,
    )(energy, *halos, share, table, sea_block, slot_owner)
    return call(
        functools.partial(gather_kernel, ring, cols),
        shape((slots, rows, lons), f32),
        [vmem] * wide,
        (pltpu.VMEM((rows, slots + SUBS, LANES), f32), pltpu.SemaphoreType.DMA((3 * rows,))),
        on_chip_result=False,
    )(*swap_blocks(updated))


def solution(mesh):
    wide = mesh.shape["wide"]

    def body(spectrum, *rest):
        slots, rows, lons = spectrum.shape
        fits = rows == SUBS and lons == LANES and wide == SUBS and slots % (3 * ROWS_AT_ONCE) == 0
        fits = fits and (slots * wide) % LANES == 0
        return (block_body if fits else general_body)(spectrum, *rest)

    return jax.shard_map(
        body,
        mesh=mesh,
        in_specs=(P("wide", "slab", None), P("slab", None), P(), P(), P()),
        out_specs=P("wide", "slab", None),
        check_vma=False,
    )
```
